32 devices in a mesh: dp: 2 (over x), tp: 4 (over z), cp: 4 (over y, core).
Axes of the slice: x: 2, y: 2, z: 4, core: 2. Of those that a mesh axis runs over, the one named last changes fastest.
Arguments:
- hidden: bfloat16 [8, 1536, 6144], P('dp', 'cp'), parts along dimension 0
- alphas: float32 [2], replicated
- wq_attn: bfloat16 [6144, 8192], P(None, 'tp')
- wk_attn: bfloat16 [6144, 1024], P(None, 'tp')
- wv_attn: bfloat16 [6144, 1024], P(None, 'tp')
- wo_attn: bfloat16 [8192, 6144], P('tp')
- gain_attn: float32 [6144], replicated
- wq_lin: bfloat16 [6144, 8192], P(None, 'tp')
- wk_lin: bfloat16 [6144, 8192], P(None, 'tp')
- wv_lin: bfloat16 [6144, 8192], P(None, 'tp')
- wg_lin: bfloat16 [6144, 8192], P(None, 'tp')
- slopes: float32 [64], P('tp')
- gain_inner: float32 [8192], P('tp')
- wo_lin: bfloat16 [8192, 6144], P('tp')
- gain_lin: float32 [6144], replicated
Outputs:
- output: bfloat16 [8, 1536, 6144], P('dp', 'cp'), parts along dimension 0
There are 2 independent parts. The reference program is written for one: setup_inputs(seed, part) draws one part's arguments, and reference() takes and returns one part's arrays. A program takes and returns all parts, laid end to end along the dimension named above; an argument that names none is the same for every part.
All inputs are finite; a program needn't handle non-finite values.
Results may differ from the reference program's by a relative error of at most 0.012291.
Values are sent between devices in bfloat16 or wider.
A program may use at most 1 GiB of HBM per device.

```python
import math
import jax
import jax.numpy as jnp
from jax import lax

BATCH = 4
SEQ = 1536
D = 6144
HEADS = 64
KV_HEADS = 8
HEAD = 128
CHUNK = 128

GROUP = HEADS // KV_HEADS
ROT = HEAD // 2
WIDTH = HEADS * HEAD
KV_WIDTH = KV_HEADS * HEAD
ROPE_BASE = 10000000.0
NORM_EPS = 1e-5


def setup_inputs(seed: int = 0, part: int = 0) -> dict:
    base_key = jax.random.key(seed)
    part_key = jax.random.fold_in(base_key, part)
    keys = jax.random.split(base_key, 16)
    logit_std = math.sqrt(max(math.log(SEQ / 8.0), 1.0))
    qk_scale = math.sqrt(logit_std / D)
    in_scale = 1.0 / math.sqrt(D)
    out_scale = 3.0 / math.sqrt(WIDTH)

    def normal_w(slot, shape, scale):
        return jax.random.normal(keys[slot], shape, jnp.float32) * scale

    head_scale = jnp.exp(jax.random.uniform(keys[0], (HEADS,), jnp.float32, -math.log(3.0), math.log(3.0)))
    rates = jnp.exp(jax.random.uniform(keys[1], (HEADS,), jnp.float32, math.log(0.25), math.log(8.0)))
    return {
        'hidden': jax.random.normal(part_key, (BATCH, SEQ, D), jnp.float32).astype(jnp.bfloat16),
        'alphas': jax.random.uniform(keys[2], (2,), jnp.float32, 1.5, 3.0),
        'wq_attn': normal_w(3, (D, WIDTH), qk_scale).astype(jnp.bfloat16),
        'wk_attn': normal_w(4, (D, KV_WIDTH), qk_scale).astype(jnp.bfloat16),
        'wv_attn': normal_w(5, (D, KV_WIDTH), in_scale).astype(jnp.bfloat16),
        'wo_attn': normal_w(6, (WIDTH, D), out_scale).astype(jnp.bfloat16),
        'gain_attn': jax.random.uniform(keys[7], (D,), jnp.float32, 0.5, 1.5),
        'wq_lin': normal_w(8, (D, WIDTH), in_scale).astype(jnp.bfloat16),
        'wk_lin': normal_w(9, (D, WIDTH), in_scale).astype(jnp.bfloat16),
        'wv_lin': (normal_w(10, (D, WIDTH), in_scale) * jnp.repeat(head_scale, HEAD)[None, :]).astype(jnp.bfloat16),
        'wg_lin': normal_w(11, (D, WIDTH), in_scale).astype(jnp.bfloat16),
        'slopes': rates / SEQ,
        'gain_inner': jax.random.uniform(keys[12], (WIDTH,), jnp.float32, 0.5, 1.5),
        'wo_lin': normal_w(13, (WIDTH, D), out_scale).astype(jnp.bfloat16),
        'gain_lin': jax.random.uniform(keys[14], (D,), jnp.float32, 0.5, 1.5),
    }


def rms_norm(values, gain_vec):
    return values * lax.rsqrt(jnp.mean(values * values, axis=-1, keepdims=True) + NORM_EPS) * gain_vec


def project(inputs, weight):
    flat_in = inputs.reshape(-1, inputs.shape[-1])
    product = jnp.dot(flat_in, weight, preferred_element_type=jnp.float32)
    return product.reshape(inputs.shape[:-1] + (weight.shape[-1],))


def rotary(values, positions):
    half = ROT // 2
    inv_freq = jnp.power(ROPE_BASE, -jnp.arange(half, dtype=jnp.float32) * 2.0 / ROT)
    angles = positions.astype(jnp.float32)[:, None] * inv_freq[None, :]
    cosine = jnp.cos(angles)[:, None, :]
    sine = jnp.sin(angles)[:, None, :]
    first = values[..., :half]
    second = values[..., half:ROT]
    return jnp.concatenate([first * cosine - second * sine, second * cosine + first * sine, values[..., ROT:]], axis=-1)


def softmax_layer(hidden, alphas, wq_attn, wk_attn, wv_attn, wo_attn, gain_attn):
    positions = jnp.arange(SEQ)
    keys_all = rotary(project(hidden, wk_attn).reshape(BATCH, SEQ, KV_HEADS, HEAD), positions).astype(jnp.bfloat16)
    values_all = project(hidden, wv_attn).astype(jnp.bfloat16).reshape(BATCH, SEQ, KV_HEADS, HEAD)
    keys_heads = jnp.moveaxis(keys_all, 2, 0)
    values_heads = jnp.moveaxis(values_all, 2, 0)
    blocks = jnp.moveaxis(hidden.reshape(BATCH, SEQ // CHUNK, CHUNK, D), 1, 0)
    starts = jnp.arange(SEQ // CHUNK) * CHUNK
    scale = 1.0 / math.sqrt(HEAD)

    def query_block(inputs):
        block, start = inputs
        q_pos = start + jnp.arange(CHUNK)
        queries = rotary(project(block, wq_attn).reshape(BATCH, CHUNK, HEADS, HEAD), q_pos).astype(jnp.bfloat16)
        queries = jnp.moveaxis(queries.reshape(BATCH, CHUNK, KV_HEADS, GROUP, HEAD), 2, 0)
        mask = q_pos[:, None] >= positions[None, :]

        def per_head(head_in):
            q_head, k_head, v_head = head_in
            scores = jnp.einsum('bqgd,bsd->bgqs', q_head.astype(jnp.float32), k_head.astype(jnp.float32)) * scale
            scores = jnp.where(mask, scores, -jnp.inf)
            prob_vals = jax.nn.softmax(scores, axis=-1).astype(jnp.bfloat16)
            return jnp.einsum('bgqs,bsd->bqgd', prob_vals.astype(jnp.float32), v_head.astype(jnp.float32))

        head_out = lax.map(per_head, (queries, keys_heads, values_heads))
        attn_out = jnp.moveaxis(head_out, 0, 2).astype(jnp.bfloat16).reshape(BATCH, CHUNK, WIDTH)
        mixed = project(attn_out, wo_attn)
        return rms_norm(alphas[0] * block.astype(jnp.float32) + mixed, gain_attn).astype(jnp.bfloat16)

    out_blocks = lax.map(query_block, (blocks, starts))
    return jnp.moveaxis(out_blocks, 0, 1).reshape(BATCH, SEQ, D)


def lightning_layer(mid_hidden, alphas, wq_lin, wk_lin, wv_lin, wg_lin, slopes, gain_inner, wo_lin, gain_lin):
    offsets = jnp.arange(CHUNK).astype(jnp.float32)
    tok_gap = offsets[:, None] - offsets[None, :]
    intra_w = jnp.where(tok_gap[None] >= 0, jnp.exp(-slopes[:, None, None] * jnp.maximum(tok_gap, 0.0)[None]), 0.0)
    query_decay = jnp.exp(-slopes[None, :] * (offsets[:, None] + 1.0))
    key_decay = jnp.exp(-slopes[None, :] * (CHUNK - 1.0 - offsets[:, None]))
    tile_decay = jnp.exp(-slopes * CHUNK)
    blocks = jnp.moveaxis(mid_hidden.reshape(BATCH, SEQ // CHUNK, CHUNK, D), 1, 0)

    def heads_of(block, weight):
        return jax.nn.silu(project(block, weight)).astype(jnp.bfloat16).astype(jnp.float32).reshape(BATCH, CHUNK, HEADS, HEAD)

    def step(state, block):
        queries = heads_of(block, wq_lin)
        keys_c = heads_of(block, wk_lin)
        values_c = heads_of(block, wv_lin)
        gate_vals = jax.nn.sigmoid(project(block, wg_lin))
        scores = jnp.einsum('bqhd,bshd->bhqs', queries, keys_c) * intra_w[None]
        inside = jnp.einsum('bhqs,bshe->bqhe', scores, values_c)
        carried = jnp.einsum('bqhd,bhde->bqhe', queries, state) * query_decay[None, :, :, None]
        mixed = (inside + carried).reshape(BATCH, CHUNK, WIDTH)
        inner_vals = (rms_norm(mixed, gain_inner) * gate_vals).astype(jnp.bfloat16)
        new_state = tile_decay[None, :, None, None] * state + jnp.einsum('bshd,bshe->bhde', keys_c * key_decay[None, :, :, None], values_c)
        lin_out = project(inner_vals, wo_lin)
        out_block = rms_norm(alphas[1] * block.astype(jnp.float32) + lin_out, gain_lin).astype(jnp.bfloat16)
        return new_state, out_block

    init_state = jnp.zeros((BATCH, HEADS, HEAD, HEAD), jnp.float32)
    out_blocks = lax.scan(step, init_state, blocks)[1]
    return jnp.moveaxis(out_blocks, 0, 1).reshape(BATCH, SEQ, D)


def reference(hidden, alphas, wq_attn, wk_attn, wv_attn, wo_attn, gain_attn, wq_lin, wk_lin, wv_lin, wg_lin, slopes, gain_inner, wo_lin, gain_lin):
    mid_hidden = softmax_layer(hidden, alphas, wq_attn, wk_attn, wv_attn, wo_attn, gain_attn)
    return lightning_layer(mid_hidden, alphas, wq_lin, wk_lin, wv_lin, wg_lin, slopes, gain_inner, wo_lin, gain_lin)
```

```python
import functools
import math

import jax
import jax.numpy as jnp
from jax import lax
from jax.experimental import pallas as pl
from jax.experimental.pallas import tpu as pltpu
from jax.sharding import PartitionSpec as P

ROPE_BASE = 10000000.0
NORM_EPS = 1e-5
HEAD = 128
MESH = pl.DeviceIdType.MESH
F32 = jnp.float32
BF16 = jnp.bfloat16
ANY = pl.BlockSpec(memory_space=pl.ANY)
VMEM = pl.BlockSpec(memory_space=pltpu.VMEM)
SMEM = pl.BlockSpec(memory_space=pltpu.SMEM)

LEAD = 2
RING = 16
UNITS = 32
W_SLOTS = 3


def dot(lhs, rhs):
    return jnp.dot(lhs, rhs, preferred_element_type=F32)


def dot_t(lhs, rhs):
    return lax.dot_general(lhs, rhs, (((1,), (1,)), ((), ())), preferred_element_type=F32)


def rotary_tables(positions):
    rot = HEAD // 2
    half = rot // 2
    inv_freq = jnp.power(ROPE_BASE, -jnp.arange(half, dtype=F32) * 2.0 / rot)
    angles = positions.astype(F32)[:, None] * inv_freq[None, :]
    cosine, sine = jnp.cos(angles), jnp.sin(angles)
    n = positions.shape[0]
    same = jnp.concatenate([cosine, cosine, jnp.ones((n, HEAD - rot), F32)], axis=1)
    from_right = jnp.concatenate([-sine, jnp.zeros((n, HEAD - half), F32)], axis=1)
    from_left = jnp.concatenate([jnp.zeros((n, half), F32), sine, jnp.zeros((n, HEAD - rot), F32)], axis=1)
    return same, from_right, from_left


def attention_kernel(scale, n_heads, q_ref, k_ref, v_ref, same_ref, right_ref, left_ref, o_ref, acc, top, total):
    blk = lax.axis_index("cp")
    n_tok = q_ref.shape[0]
    quarter = HEAD // 4

    def head(h, carry):
        cols = pl.ds(pl.multiple_of(h * HEAD, HEAD), HEAD)
        raw = q_ref[:, cols]
        turned = raw * same_ref[...] + pltpu.roll(raw, HEAD - quarter, 1) * right_ref[...]
        query = (turned + pltpu.roll(raw, quarter, 1) * left_ref[...]).astype(BF16)

        scores = dot_t(query, k_ref[blk]) * scale
        rows = lax.broadcasted_iota(jnp.int32, scores.shape, 0)
        keys = lax.broadcasted_iota(jnp.int32, scores.shape, 1)
        scores = jnp.where(rows >= keys, scores, -jnp.inf)
        peak = jnp.max(scores, axis=-1, keepdims=True)
        probs = jnp.exp(scores - peak)
        top[...] = jnp.broadcast_to(peak, (n_tok, HEAD))
        total[...] = jnp.broadcast_to(jnp.sum(probs, axis=-1, keepdims=True), (n_tok, HEAD))
        acc[...] = dot(probs.astype(BF16), v_ref[blk])

        def earlier(j, inner):
            later_scores = dot_t(query, k_ref[j]) * scale
            old = top[:, 0:1]
            new = jnp.maximum(old, jnp.max(later_scores, axis=-1, keepdims=True))
            factor = jnp.exp(old - new)
            vals = jnp.exp(later_scores - new)
            top[...] = jnp.broadcast_to(new, (n_tok, HEAD))
            total[...] = total[...] * factor + jnp.sum(vals, axis=-1, keepdims=True)
            acc[...] = acc[...] * factor + dot(vals.astype(BF16), v_ref[j])
            return inner

        lax.fori_loop(0, blk, earlier, 0)
        o_ref[:, cols] = (acc[...] / total[...]).astype(BF16)
        return carry

    lax.fori_loop(0, n_heads, head, 0)


def attention(q_proj, kv_all, tables, n_tok):
    n_rows, width = q_proj.shape
    n_batch = n_rows // n_tok
    n_cp = kv_all.shape[0]
    kv_heads = kv_all.shape[3] // (2 * HEAD)
    per_kv = width // kv_heads
    table = pl.BlockSpec((n_tok, HEAD), lambda b, g: (0, 0))
    return pl.pallas_call(
        functools.partial(attention_kernel, 1.0 / math.sqrt(HEAD), per_kv // HEAD),
        out_shape=jax.ShapeDtypeStruct((n_rows, width), BF16),
        grid=(n_batch, kv_heads),
        in_specs=[
            pl.BlockSpec((n_tok, per_kv), lambda b, g: (b, g)),
            pl.BlockSpec((n_cp, None, n_tok, HEAD), lambda b, g: (0, b, 0, g)),
            pl.BlockSpec((n_cp, None, n_tok, HEAD), lambda b, g: (0, b, 0, kv_heads + g)),
            table,
            table,
            table,
        ],
        out_specs=pl.BlockSpec((n_tok, per_kv), lambda b, g: (b, g)),
        scratch_shapes=[pltpu.VMEM((n_tok, HEAD), F32)] * 3,
        compiler_params=pltpu.CompilerParams(vmem_limit_bytes=48 * 1024 * 1024),
        cost_estimate=pl.CostEstimate(flops=2 * n_rows * width * n_tok * 5, bytes_accessed=n_rows * width * 6, transcendentals=0),
    )(q_proj, kv_all, kv_all, *tables)


def fused_kernel(
    n_tp,
    n_cp,
    att,
    hid,
    wo_a,
    wk,
    wv,
    wq,
    wg,
    wo_l,
    gains,
    ginner,
    alphas,
    slopes,
    out,
    h1,
    part,
    summed,
    normed,
    w_buf,
    wo_buf,
    y_buf,
    kvq,
    gate,
    o_buf,
    state,
    state_in,
    res,
    wide,
    acc,
    sq_acc,
    row_inv,
    sq_send,
    sq_recv,
    reduce_send,
    reduce_recv,
    back_send,
    back_recv,
    res_sem,
    out_sem,
    w_sem,
    wo_sem,
    y_sem,
    state_send,
    state_recv,
    sq_send_sem,
    sq_recv_sem,
    credit,
):
    _, n_tok, model = part.shape
    width = y_buf.shape[1]
    n_heads = width // HEAD
    n_batch = att.shape[0] // n_tok
    half = n_tok // 2
    rows = res.shape[2]
    per_batch = half // rows
    per_group = per_batch // 4
    layer_pieces = n_batch * per_batch
    pieces = 2 * layer_pieces
    w_cols = w_buf.shape[2]
    wo_cols = wo_buf.shape[2]
    n_wo = model // wo_cols
    last = n_tp - 1
    trip = 2 * last * LEAD
    z = lax.axis_index("tp")
    c = lax.axis_index("cp")

    barrier = pltpu.get_barrier_semaphore()
    for k in range(1, n_tp):
        pl.semaphore_signal(barrier, inc=1, device_id={"tp": lax.rem(z + k, n_tp)}, device_id_type=MESH)

    @pl.when(c > 0)
    def _():
        pl.semaphore_signal(barrier, inc=1, device_id={"cp": c - 1}, device_id_type=MESH)

    @pl.when(c < n_cp - 1)
    def _():
        pl.semaphore_signal(barrier, inc=1, device_id={"cp": c + 1}, device_id_type=MESH)

    inner = (c > 0) & (c < n_cp - 1)

    @pl.when(inner)
    def _():
        pl.semaphore_wait(barrier, n_tp + 1)

    @pl.when(jnp.logical_not(inner))
    def _():
        pl.semaphore_wait(barrier, n_tp)

    def row_of(g, f):
        return pl.multiple_of(f * half + lax.rem(g, per_batch) * rows, rows)

    def view(ref, g, f):
        return ref.at[lax.rem(lax.div(g, per_batch), 2), pl.ds(row_of(g, f), rows), :]

    def place(f):
        return (z, z + 1, z - 1) if f == 0 else (last - z, z - 1, z + 1)

    def forward(g, f):
        slot = lax.rem(g, RING)
        return pltpu.make_async_remote_copy(
            src_ref=view(part, g, f),
            dst_ref=view(summed, g, f),
            send_sem=reduce_send.at[f, slot],
            recv_sem=reduce_recv.at[f, slot],
            device_id={"tp": place(f)[1]},
            device_id_type=MESH,
        )

    def backward(g, f):
        slot = lax.rem(g, RING)
        return pltpu.make_async_remote_copy(
            src_ref=view(summed, g, f),
            dst_ref=view(summed, g, f),
            send_sem=back_send.at[f, slot],
            recv_sem=back_recv.at[f, slot],
            device_id={"tp": place(f)[2]},
            device_id_type=MESH,
        )

    def hbm_rows(ref, g, f):
        batch = lax.rem(lax.div(g, per_batch), n_batch)
        return ref.at[pl.ds(pl.multiple_of(batch * n_tok + row_of(g, f), rows), rows), :]

    def res_copy(g, f, ref):
        slot = lax.rem(g, 4)
        return pltpu.make_async_copy(hbm_rows(ref, g, f), res.at[f, slot], res_sem.at[f, slot])

    def out_copy(g, f, ref):
        return pltpu.make_async_copy(view(normed, g, f), hbm_rows(ref, g, f), out_sem.at[f, lax.rem(g, 4)])

    def norm_rows(g, f):
        layer = (g >= layer_pieces).astype(jnp.int32)
        slot = lax.rem(g, 4)
        at = lax.rem(lax.div(g, per_batch), 2)
        span = pl.ds(row_of(g, f), rows)
        alpha = alphas[layer]
        n_chunk = model // wo_cols

        def first(i, sq):
            cols = pl.ds(pl.multiple_of(i * wo_cols, wo_cols), wo_cols)
            vals = alpha * res[f, slot, :, cols].astype(F32) + summed[at, span, cols].astype(F32)
            wide[:, cols] = vals
            return sq + vals * vals

        sq = lax.fori_loop(0, n_chunk, first, jnp.zeros((rows, wo_cols), F32))
        scale = lax.rsqrt(jnp.sum(sq, axis=-1, keepdims=True) / model + NORM_EPS)

        def second(i, carry):
            cols = pl.ds(pl.multiple_of(i * wo_cols, wo_cols), wo_cols)
            normed[at, span, cols] = (wide[:, cols] * scale * gains[layer, :, cols]).astype(BF16)
            return carry

        lax.fori_loop(0, n_chunk, second, 0)

    def known(g):
        return (g >= 0) & (g < pieces)

    def service(step):
        ahead = step + 3 - trip
        for f in range(2):

            @pl.when((ahead >= 0) & (ahead < layer_pieces))
            def _():
                res_copy(ahead, f, hid).start()

            @pl.when((ahead >= layer_pieces) & (ahead < pieces))
            def _():
                res_copy(ahead, f, h1).start()

        for f in range(2):
            pos = place(f)[0]
            g = step - LEAD * pos

            @pl.when(known(g) & (pos > 0))
            def _():
                forward(g, f).wait_recv()

            @pl.when(known(g) & (pos > 0) & (pos < last))
            def _():
                at = lax.rem(lax.div(g, per_batch), 2)
                span = pl.ds(row_of(g, f), rows)
                part[at, span, :] = part[at, span, :] + summed[at, span, :]

            @pl.when(known(g) & (pos == last))
            def _():
                at = lax.rem(lax.div(g, per_batch), 2)
                span = pl.ds(row_of(g, f), rows)
                summed[at, span, :] = part[at, span, :] + summed[at, span, :]

        for f in range(2):
            pos = place(f)[0]
            g = step - LEAD * pos

            @pl.when(known(g) & (pos < last))
            def _():
                forward(g, f).start()

            @pl.when(known(g) & (pos == last))
            def _():
                backward(g, f).start()

        for f in range(2):
            pos = place(f)[0]
            g = step - LEAD * (2 * last - pos)

            @pl.when(known(g) & (pos < last))
            def _():
                backward(g, f).wait_recv()

            @pl.when(known(g) & (pos < last) & (pos > 0))
            def _():
                backward(g, f).start()

        for f in range(2):
            pos = place(f)[0]
            sent = step - (LEAD * (last - 1) + 3)

            @pl.when(known(sent) & (pos < last))
            def _():
                forward(sent, f).wait_send()

        done = step - trip

        @pl.when(known(done))
        def _():
            for f in range(2):
                pos = place(f)[0]

                @pl.when(pos > 0)
                def _():
                    backward(done, f).wait_send()

                @pl.when(done < layer_pieces)
                def _():
                    res_copy(done, f, hid).wait()

                @pl.when(done >= layer_pieces)
                def _():
                    res_copy(done, f, h1).wait()

                @pl.when(done >= 4)
                def _():
                    out_copy(done - 4, f, out).wait()

                norm_rows(done, f)

                @pl.when(done < layer_pieces)
                def _():
                    out_copy(done, f, h1).start()

                @pl.when(done >= layer_pieces)
                def _():
                    out_copy(done, f, out).start()

    projections = (wk, wv, wq, wg)

    def w_copy(which, tile, slot):
        cols = pl.ds(pl.multiple_of(tile * w_cols, w_cols), w_cols)
        return pltpu.make_async_copy(projections[which].at[:, cols], w_buf.at[slot], w_sem.at[slot])

    def wo_copy(weight, tile):
        cols = pl.ds(pl.multiple_of(tile * wo_cols, wo_cols), wo_cols)
        slot = lax.rem(tile, 2)
        return pltpu.make_async_copy(weight.at[:, cols], wo_buf.at[slot], wo_sem.at[slot])

    def has_projection(phase):
        return (phase >= 2) & (phase < 2 + n_batch)

    def project(unit, phase, which, tile):
        slot = lax.rem(unit, W_SLOTS)
        w_copy(0, tile, slot).wait()
        at = lax.rem(phase, 2)
        depth = model // 6
        acc[:, 0:w_cols] = jnp.zeros((n_tok, w_cols), F32)

        def chunk(i, carry):
            ks = pl.ds(pl.multiple_of(i * depth, depth), depth)
            acc[:, 0:w_cols] += dot(normed[at, :, ks], w_buf[slot, ks, :])
            return carry

        lax.fori_loop(0, 6, chunk, 0)
        cols = pl.ds(pl.multiple_of(tile * w_cols, w_cols), w_cols)
        vals = acc[:, 0:w_cols]
        soft = jax.nn.sigmoid(vals)

        @pl.when(which < 3)
        def _():
            kvq[which, :, cols] = (vals * soft).astype(BF16)

        @pl.when(which == 3)
        def _():
            gate[:, cols] = soft

    def out_project(phase, tile):
        wo_copy(wo_a, tile).wait()
        slot = lax.rem(tile, 2)
        cols = pl.ds(pl.multiple_of(tile * wo_cols, wo_cols), wo_cols)
        at = lax.rem(phase + 1, 2)
        part[at, :, cols] = dot(y_buf[...], wo_buf[slot]).astype(BF16)

    def state_copy():
        return pltpu.make_async_remote_copy(
            src_ref=state,
            dst_ref=state_in,
            send_sem=state_send,
            recv_sem=state_recv,
            device_id={"cp": c + 1},
            device_id_type=MESH,
        )

    def local_lightning():
        def head(h, carry):
            cols = pl.ds(pl.multiple_of(h * HEAD, HEAD), HEAD)
            rate = slopes[h]
            key, value, query = kvq[0, :, cols], kvq[1, :, cols], kvq[2, :, cols]
            scores = dot_t(query, key)
            gap = lax.broadcasted_iota(jnp.int32, scores.shape, 0) - lax.broadcasted_iota(jnp.int32, scores.shape, 1)
            decay = jnp.where(gap >= 0, jnp.exp(-rate * gap.astype(F32)), 0.0)
            o_buf[:, cols] = dot((scores * decay).astype(BF16), value)
            to_end = (n_tok - 1 - lax.broadcasted_iota(jnp.int32, (n_tok, HEAD), 0)).astype(F32)
            faded = key.astype(F32) * jnp.exp(-rate * to_end)
            state[h] = dot(faded.T.astype(BF16), value)
            return carry

        lax.fori_loop(0, n_heads, head, 0)

    def add_incoming():
        def head(h, carry):
            state[h] = state_in[h] * jnp.exp(jnp.zeros((HEAD, HEAD), F32) - slopes[h] * n_tok) + state[h]
            return carry

        lax.fori_loop(0, n_heads, head, 0)

    def send_state(batch):
        @pl.when(batch > 0)
        def _():
            pl.semaphore_wait(credit, 1)

        state_copy().start()

    def sq_copy(batch, k):
        peer = lax.rem(z + k, n_tp)
        return pltpu.make_async_remote_copy(
            src_ref=sq_send,
            dst_ref=sq_recv.at[batch, z],
            send_sem=sq_send_sem.at[k],
            recv_sem=sq_recv_sem.at[batch, z],
            device_id={"tp": peer},
            device_id_type=MESH,
        )

    def sq_arrival(batch, k):
        source = lax.rem(z + n_tp - k, n_tp)
        return pltpu.make_async_remote_copy(
            src_ref=sq_send,
            dst_ref=sq_recv.at[batch, source],
            send_sem=sq_send_sem.at[k],
            recv_sem=sq_recv_sem.at[batch, source],
            device_id={"tp": source},
            device_id_type=MESH,
        )

    def add_earlier(batch):
        @pl.when(c == n_cp - 1)
        def _():
            state_copy().wait_recv()

        @pl.when(c < n_cp - 1)
        def _():
            state_copy().wait_send()

        sq_acc[...] = jnp.zeros_like(sq_acc)

        def head(h, carry):
            cols = pl.ds(pl.multiple_of(h * HEAD, HEAD), HEAD)

            @pl.when(c > 0)
            def _():
                steps = (lax.broadcasted_iota(jnp.int32, (n_tok, HEAD), 0) + 1).astype(F32)
                prior = dot(kvq[2, :, cols], state_in[h].astype(BF16))
                o_buf[:, cols] += prior * jnp.exp(-slopes[h] * steps)

            vals = o_buf[:, cols]
            sq_acc[...] += vals * vals
            return carry

        lax.fori_loop(0, n_heads, head, 0)

        @pl.when((c > 0) & (batch < n_batch - 1))
        def _():
            pl.semaphore_signal(credit, inc=1, device_id={"cp": c - 1}, device_id_type=MESH)

        row_sq = jnp.broadcast_to(jnp.sum(sq_acc[...], axis=-1, keepdims=True), (n_tok, HEAD))
        sq_send[...] = row_sq.T[0:8, :]
        sq_recv[batch, z] = sq_send[...]
        for k in range(1, n_tp):
            sq_copy(batch, k).start()

    def finish_lightning(batch):
        for k in range(1, n_tp):
            sq_arrival(batch, k).wait_recv()
        for k in range(1, n_tp):
            sq_copy(batch, k).wait_send()
        total = sq_recv[batch, 0]
        for k in range(1, n_tp):
            total = total + sq_recv[batch, k]
        tall = jnp.broadcast_to(total[0:1, :], (HEAD, n_tok)).T
        row_inv[...] = lax.rsqrt(tall / (width * n_tp) + NORM_EPS)

        def head(h, carry):
            cols = pl.ds(pl.multiple_of(h * HEAD, HEAD), HEAD)
            y_buf[:, cols] = (o_buf[:, cols] * row_inv[...] * ginner[h] * gate[:, cols]).astype(BF16)
            return carry

        lax.fori_loop(0, n_heads, head, 0)

    def unit_body(unit, carry):
        phase = lax.div(unit, UNITS) - 1
        r = lax.rem(unit, UNITS)
        which = lax.div(r, 8)
        tile = lax.rem(r, 8)
        first_layer = phase < n_batch - 1
        second_layer = (phase >= 3) & (phase < 3 + n_batch)
        projects = has_projection(phase)

        @pl.when(lax.rem(tile, 3) == 0)
        def _():
            part_of = lax.div(tile, 3)

            def one(i, inner):
                service(phase * per_batch + which * per_group + part_of * (per_group // 3) + i)
                return inner

            if per_group == 3:
                one(0, 0)
            else:
                lax.fori_loop(0, per_group // 3, one, 0)

        @pl.when((r == 8) & first_layer)
        def _():
            batch_rows = pl.ds(pl.multiple_of((phase + 1) * n_tok, n_tok), n_tok)
            pltpu.make_async_copy(att.at[batch_rows, :], y_buf, y_sem).start()

        for i in range(2):

            @pl.when((r == 8 + i) & first_layer)
            def _():
                wo_copy(wo_a, i).start()

            @pl.when((r == 8 + i) & second_layer)
            def _():
                wo_copy(wo_l, i).start()

        @pl.when((r == 4) & second_layer & (c == 2))
        def _():
            state_copy().wait_recv()
            add_incoming()
            send_state(phase - 3)

        @pl.when((r == 12) & second_layer)
        def _():
            add_earlier(phase - 3)

        @pl.when((r == 16) & second_layer)
        def _():
            finish_lightning(phase - 3)

        @pl.when((r == 16) & first_layer)
        def _():
            pltpu.make_async_copy(att.at[pl.ds(0, n_tok), :], y_buf, y_sem).wait()

        wo_tile = r - 16

        @pl.when((wo_tile >= 0) & (wo_tile < n_wo) & (first_layer | second_layer))
        def _():
            out_project(phase, wo_tile)

            @pl.when((wo_tile < n_wo - 2) & first_layer)
            def _():
                wo_copy(wo_a, wo_tile + 2).start()

            @pl.when((wo_tile < n_wo - 2) & second_layer)
            def _():
                wo_copy(wo_l, wo_tile + 2).start()

        @pl.when(projects)
        def _():
            project(unit, phase, which, tile)

        coming = unit + W_SLOTS
        coming_r = lax.rem(coming, UNITS)

        @pl.when(has_projection(lax.div(coming, UNITS) - 1))
        def _():
            for k in range(4):

                @pl.when(lax.div(coming_r, 8) == k)
                def _():
                    w_copy(k, lax.rem(coming_r, 8), lax.rem(coming, W_SLOTS)).start()

        @pl.when((r == 23) & projects)
        def _():
            local_lightning()

            @pl.when(c == 0)
            def _():
                send_state(phase - 2)

        @pl.when((r == 28) & projects & (c == 1))
        def _():
            state_copy().wait_recv()
            add_incoming()
            send_state(phase - 2)

        return carry

    n_phases = 2 * n_batch + 2
    lax.fori_loop(0, n_phases * UNITS, unit_body, 0)
    for f in range(2):
        for k in range(4):
            out_copy(pieces - 4 + k, f, out).wait()


def fused_layers(att, hid, weights, gains, ginner, alphas, slopes, n_tok, n_tp, n_cp):
    wo_a, wk, wv, wq, wg, wo_l = weights
    n_rows, width = att.shape
    model = hid.shape[1]
    n_batch = n_rows // n_tok
    n_heads = width // HEAD
    rows = n_tok // 24
    w_cols = width // 8
    wo_cols = model // 12
    vmem, dma = pltpu.VMEM, pltpu.SemaphoreType.DMA
    scratch = [
        vmem((2, n_tok, model), BF16),
        vmem((2, n_tok, model), BF16),
        vmem((2, n_tok, model), BF16),
        vmem((W_SLOTS, model, w_cols), BF16),
        vmem((2, width, wo_cols), BF16),
        vmem((n_tok, width), BF16),
        vmem((3, n_tok, width), BF16),
        vmem((n_tok, width), F32),
        vmem((n_tok, width), F32),
        vmem((n_heads, HEAD, HEAD), F32),
        vmem((n_heads, HEAD, HEAD), F32),
        vmem((2, 4, rows, model), BF16),
        vmem((rows, model), F32),
        vmem((n_tok, max(w_cols, HEAD)), F32),
        vmem((n_tok, HEAD), F32),
        vmem((n_tok, HEAD), F32),
        vmem((8, n_tok), F32),
        vmem((n_batch, n_tp, 8, n_tok), F32),
        dma((2, RING)),
        dma((2, RING)),
        dma((2, RING)),
        dma((2, RING)),
        dma((2, 4)),
        dma((2, 4)),
        dma((W_SLOTS,)),
        dma((2,)),
        dma,
        dma,
        dma,
        dma((n_tp,)),
        dma((n_batch, n_tp)),
        pltpu.SemaphoreType.REGULAR,
    ]
    flops = 2 * n_rows * model * width * 6
    return pl.pallas_call(
        functools.partial(fused_kernel, n_tp, n_cp),
        out_shape=[jax.ShapeDtypeStruct((n_rows, model), BF16)] * 2,
        in_specs=[ANY] * 8 + [VMEM] * 2 + [SMEM] * 2,
        out_specs=[ANY] * 2,
        scratch_shapes=scratch,
        compiler_params=pltpu.CompilerParams(collective_id=0, has_side_effects=True, vmem_limit_bytes=67043328),
        cost_estimate=pl.CostEstimate(flops=flops, bytes_accessed=12 * n_rows * model, transcendentals=0),
    )(att, hid, wo_a, wk, wv, wq, wg, wo_l, gains, ginner, alphas, slopes)


def solution(mesh):
    n_tp, n_cp = mesh.shape["tp"], mesh.shape["cp"]

    def body(hidden, alphas, wq_attn, wk_attn, wv_attn, wo_attn, gain_attn, wq_lin, wk_lin, wv_lin, wg_lin, slopes, gain_inner, wo_lin, gain_lin):
        n_batch, n_tok, model = hidden.shape
        flat = hidden.reshape(n_batch * n_tok, model)
        kv_width = wk_attn.shape[1]
        positions = lax.axis_index("cp") * n_tok + jnp.arange(n_tok)
        tables = rotary_tables(positions)

        k_proj = dot(flat, wk_attn).reshape(n_batch, n_tok, kv_width // HEAD, HEAD)
        same, from_right, from_left = (t[None, :, None, :] for t in tables)
        quarter = HEAD // 4
        keys = k_proj * same + jnp.roll(k_proj, -quarter, axis=-1) * from_right + jnp.roll(k_proj, quarter, axis=-1) * from_left
        keys = keys.astype(BF16).reshape(n_batch, n_tok, kv_width)
        values = dot(flat, wv_attn).astype(BF16).reshape(n_batch, n_tok, kv_width)
        kv_all = lax.all_gather(jnp.concatenate([keys, values], axis=-1), "cp")

        q_proj = dot(flat, wq_attn)
        att = attention(q_proj, kv_all, tables, n_tok)
        gains = jnp.stack([gain_attn, gain_lin])[:, None, :]
        weights = (wo_attn, wk_lin, wv_lin, wq_lin, wg_lin, wo_lin)
        out, _ = fused_layers(att, flat, weights, gains, gain_inner.reshape(-1, 1, HEAD), alphas, slopes, n_tok, n_tp, n_cp)
        return out.reshape(hidden.shape)

    act_spec = P("dp", "cp", None)
    rep_spec = P()
    col_spec = P(None, "tp")
    row_spec = P("tp", None)
    vec_spec = P("tp")
    in_specs = (act_spec, rep_spec, col_spec, col_spec, col_spec, row_spec, rep_spec, col_spec, col_spec, col_spec, col_spec, vec_spec, vec_spec, row_spec, rep_spec)
    return jax.shard_map(body, mesh=mesh, in_specs=in_specs, out_specs=act_spec, check_vma=False)
```

```python
import functools
import math

import jax
import jax.numpy as jnp
import numpy as np
from jax import lax
from jax.experimental import pallas as pl
from jax.experimental.pallas import tpu as pltpu
from jax.sharding import PartitionSpec as P

ROPE_BASE = 10000000.0
NORM_EPS = 1e-5
HEAD = 128
MESH = pl.DeviceIdType.MESH
F32 = jnp.float32
BF16 = jnp.bfloat16
ANY = pl.BlockSpec(memory_space=pl.ANY)
VMEM = pl.BlockSpec(memory_space=pltpu.VMEM)
SMEM = pl.BlockSpec(memory_space=pltpu.SMEM)

LEAD = 2
RING = 16
UNITS = 32
W_SLOTS = 3


def dot(lhs, rhs):
    return jnp.dot(lhs, rhs, preferred_element_type=F32)


def dot_t(lhs, rhs):
    return lax.dot_general(lhs, rhs, (((1,), (1,)), ((), ())), preferred_element_type=F32)


def rotary_table(n_pos):
    half = HEAD // 4
    inv_freq = np.power(ROPE_BASE, -np.arange(half) * 2.0 / (2 * half)).astype(np.float32)
    angles = (np.arange(n_pos, dtype=np.float32)[:, None] * inv_freq[None, :]).astype(np.float64)
    cosine, sine = np.cos(angles), np.sin(angles)
    return np.concatenate([cosine, cosine, sine, sine], axis=1).astype(np.float32)


def fold(vals, op, reduce, share):
    n_cols = vals.shape[1]
    if n_cols % HEAD:
        return jnp.broadcast_to(reduce(vals, axis=-1, keepdims=True) * share, (vals.shape[0], HEAD))
    out = vals[:, 0:HEAD]
    for k in range(1, n_cols // HEAD):
        out = op(out, vals[:, k * HEAD : (k + 1) * HEAD])
    return out


def fused_kernel(
    n_tp,
    n_cp,
    hid,
    wk_a,
    wv_a,
    wq_a,
    wo_a,
    wk,
    wv,
    wq,
    wg,
    wo_l,
    table,
    gains,
    ginner,
    alphas,
    slopes,
    out,
    h1,
    kv_all,
    part,
    summed,
    normed,
    w_buf,
    wo_buf,
    y_buf,
    kvq,
    gate,
    o_buf,
    state,
    state_in,
    res,
    wide,
    acc,
    sq_acc,
    row_inv,
    sq_send,
    sq_recv,
    kv_own,
    kv_buf,
    rope,
    sums,
    reduce_send,
    reduce_recv,
    back_send,
    back_recv,
    res_sem,
    out_sem,
    w_sem,
    wo_sem,
    hid_sem,
    rope_sem,
    kv_send,
    kv_recv,
    kv_load,
    state_send,
    state_recv,
    sq_send_sem,
    sq_recv_sem,
    credit,
):
    _, n_tok, model = part.shape
    width = y_buf.shape[1]
    n_heads = width // HEAD
    n_batch = hid.shape[0] // n_tok
    kv_width = wk_a.shape[1]
    group = width // kv_width
    n_pairs = n_heads // 2
    half = n_tok // 2
    rows = res.shape[2]
    per_batch = half // rows
    per_group = per_batch // 4
    layer_pieces = n_batch * per_batch
    pieces = 2 * layer_pieces
    w_cols = w_buf.shape[2]
    wo_cols = wo_buf.shape[2]
    n_wo = model // wo_cols
    kv_tiles = kv_width // w_cols
    a_tiles = 2 * kv_tiles + 8
    last = n_tp - 1
    trip = 2 * last * LEAD
    z = lax.axis_index("tp")
    c = lax.axis_index("cp")

    def hidden_copy(batch):
        at = lax.rem(batch, 2)
        return pltpu.make_async_copy(hid.at[pl.ds(pl.multiple_of(batch * n_tok, n_tok), n_tok), :], normed.at[at], hid_sem.at[at])

    def a_tile(unit):
        phase = lax.div(unit, UNITS) - 1
        r = lax.rem(unit, UNITS)
        late = r >= 12
        j = jnp.where(late, r - 12, r)
        is_a = (phase <= 1) & (j < a_tiles) & (jnp.logical_not(late) | (phase == 0))
        batch = jnp.where(phase == 1, 3, jnp.where(late, 2, phase + 1))
        return is_a, batch, j

    def w_cut(weight, tile, slot):
        cols = pl.ds(pl.multiple_of(tile * w_cols, w_cols), w_cols)
        return pltpu.make_async_copy(weight.at[:, cols], w_buf.at[slot], w_sem.at[slot])

    def fetch(unit):
        slot = lax.rem(unit, W_SLOTS)
        r = lax.rem(unit, UNITS)
        is_a, _, j = a_tile(unit)

        @pl.when(is_a & (j < kv_tiles))
        def _():
            w_cut(wk_a, j, slot).start()

        @pl.when(is_a & (j >= kv_tiles) & (j < 2 * kv_tiles))
        def _():
            w_cut(wv_a, j - kv_tiles, slot).start()

        @pl.when(is_a & (j >= 2 * kv_tiles))
        def _():
            w_cut(wq_a, j - 2 * kv_tiles, slot).start()

        @pl.when(has_projection(lax.div(unit, UNITS) - 1))
        def _():
            for k, weight in enumerate((wk, wv, wq, wg)):

                @pl.when(lax.div(r, 8) == k)
                def _():
                    w_cut(weight, lax.rem(r, 8), slot).start()

    def has_projection(phase):
        return (phase >= 2) & (phase < 2 + n_batch)

    for i in range(2):
        hidden_copy(i).start()
    for i in range(W_SLOTS):
        fetch(jnp.int32(i))
    table_copy = pltpu.make_async_copy(table.at[pl.ds(pl.multiple_of(c * n_tok, n_tok), n_tok), :], rope.at[0], rope_sem)
    table_copy.start()

    barrier = pltpu.get_barrier_semaphore()
    for k in range(1, n_tp):
        pl.semaphore_signal(barrier, inc=1, device_id={"tp": lax.rem(z + k, n_tp)}, device_id_type=MESH)
    for k in range(1, n_cp):
        pl.semaphore_signal(barrier, inc=1, device_id={"cp": lax.rem(c + k, n_cp)}, device_id_type=MESH)

    table_copy.wait()
    lane = lax.broadcasted_iota(jnp.int32, (n_tok, HEAD), 1)
    cosines = rope[0]
    sines = pltpu.roll(cosines, HEAD // 2, 1)
    rope[0] = jnp.where(lane < HEAD // 2, cosines, 1.0)
    rope[1] = jnp.where(lane < HEAD // 4, -sines, 0.0)
    rope[2] = jnp.where((lane >= HEAD // 4) & (lane < HEAD // 2), sines, 0.0)
    pl.semaphore_wait(barrier, n_tp + n_cp - 2)

    def row_of(g, f):
        return pl.multiple_of(f * half + lax.rem(g, per_batch) * rows, rows)

    def view(ref, g, f):
        return ref.at[lax.rem(lax.div(g, per_batch), 2), pl.ds(row_of(g, f), rows), :]

    def place(f):
        return (z, z + 1, z - 1) if f == 0 else (last - z, z - 1, z + 1)

    def forward(g, f):
        slot = lax.rem(g, RING)
        return pltpu.make_async_remote_copy(
            src_ref=view(part, g, f),
            dst_ref=view(summed, g, f),
            send_sem=reduce_send.at[f, slot],
            recv_sem=reduce_recv.at[f, slot],
            device_id={"tp": place(f)[1]},
            device_id_type=MESH,
        )

    def backward(g, f):
        slot = lax.rem(g, RING)
        return pltpu.make_async_remote_copy(
            src_ref=view(summed, g, f),
            dst_ref=view(summed, g, f),
            send_sem=back_send.at[f, slot],
            recv_sem=back_recv.at[f, slot],
            device_id={"tp": place(f)[2]},
            device_id_type=MESH,
        )

    def hbm_rows(ref, g, f):
        batch = lax.rem(lax.div(g, per_batch), n_batch)
        return ref.at[pl.ds(pl.multiple_of(batch * n_tok + row_of(g, f), rows), rows), :]

    def res_copy(g, f, ref):
        slot = lax.rem(g, 4)
        return pltpu.make_async_copy(hbm_rows(ref, g, f), res.at[f, slot], res_sem.at[f, slot])

    def out_copy(g, f, ref):
        return pltpu.make_async_copy(view(normed, g, f), hbm_rows(ref, g, f), out_sem.at[f, lax.rem(g, 4)])

    def norm_rows(g, f):
        layer = (g >= layer_pieces).astype(jnp.int32)
        slot = lax.rem(g, 4)
        at = lax.rem(lax.div(g, per_batch), 2)
        span = pl.ds(row_of(g, f), rows)
        alpha = alphas[layer]
        n_chunk = model // wo_cols

        def first(i, sq):
            cols = pl.ds(pl.multiple_of(i * wo_cols, wo_cols), wo_cols)
            vals = alpha * res[f, slot, :, cols].astype(F32) + summed[at, span, cols].astype(F32)
            wide[:, cols] = vals
            return sq + vals * vals

        sq = lax.fori_loop(0, n_chunk, first, jnp.zeros((rows, wo_cols), F32))
        scale = lax.rsqrt(jnp.sum(sq, axis=-1, keepdims=True) / model + NORM_EPS)

        def second(i, carry):
            cols = pl.ds(pl.multiple_of(i * wo_cols, wo_cols), wo_cols)
            normed[at, span, cols] = (wide[:, cols] * scale * gains[layer, :, cols]).astype(BF16)
            return carry

        lax.fori_loop(0, n_chunk, second, 0)

    def known(g):
        return (g >= 0) & (g < pieces)

    def service(step):
        ahead = step + 3 - trip
        for f in range(2):

            @pl.when((ahead >= 0) & (ahead < layer_pieces))
            def _():
                res_copy(ahead, f, hid).start()

            @pl.when((ahead >= layer_pieces) & (ahead < pieces))
            def _():
                res_copy(ahead, f, h1).start()

        for f in range(2):
            pos = place(f)[0]
            g = step - LEAD * pos

            @pl.when(known(g) & (pos > 0))
            def _():
                forward(g, f).wait_recv()

            @pl.when(known(g) & (pos > 0) & (pos < last))
            def _():
                at = lax.rem(lax.div(g, per_batch), 2)
                span = pl.ds(row_of(g, f), rows)
                part[at, span, :] = part[at, span, :] + summed[at, span, :]

            @pl.when(known(g) & (pos == last))
            def _():
                at = lax.rem(lax.div(g, per_batch), 2)
                span = pl.ds(row_of(g, f), rows)
                summed[at, span, :] = part[at, span, :] + summed[at, span, :]

        for f in range(2):
            pos = place(f)[0]
            g = step - LEAD * pos

            @pl.when(known(g) & (pos < last))
            def _():
                forward(g, f).start()

            @pl.when(known(g) & (pos == last))
            def _():
                backward(g, f).start()

        for f in range(2):
            pos = place(f)[0]
            g = step - LEAD * (2 * last - pos)

            @pl.when(known(g) & (pos < last))
            def _():
                backward(g, f).wait_recv()

            @pl.when(known(g) & (pos < last) & (pos > 0))
            def _():
                backward(g, f).start()

        for f in range(2):
            pos = place(f)[0]
            sent = step - (LEAD * (last - 1) + 3)

            @pl.when(known(sent) & (pos < last))
            def _():
                forward(sent, f).wait_send()

        done = step - trip

        @pl.when(known(done))
        def _():
            for f in range(2):
                pos = place(f)[0]

                @pl.when(pos > 0)
                def _():
                    backward(done, f).wait_send()

                @pl.when(done < layer_pieces)
                def _():
                    res_copy(done, f, hid).wait()

                @pl.when(done >= layer_pieces)
                def _():
                    res_copy(done, f, h1).wait()

                @pl.when(done >= 4)
                def _():
                    out_copy(done - 4, f, out).wait()

                norm_rows(done, f)

                @pl.when(done < layer_pieces)
                def _():
                    out_copy(done, f, h1).start()

                @pl.when(done >= layer_pieces)
                def _():
                    out_copy(done, f, out).start()

    def wo_copy(weight, tile):
        cols = pl.ds(pl.multiple_of(tile * wo_cols, wo_cols), wo_cols)
        slot = lax.rem(tile, 2)
        return pltpu.make_async_copy(weight.at[:, cols], wo_buf.at[slot], wo_sem.at[slot])

    def project(unit, at):
        slot = lax.rem(unit, W_SLOTS)
        w_cut(wk, 0, slot).wait()
        depth = model // 6
        acc[...] = jnp.zeros_like(acc)

        def chunk(i, carry):
            ks = pl.ds(pl.multiple_of(i * depth, depth), depth)
            acc[...] += dot(normed[at, :, ks], w_buf[slot, ks, :])
            return carry

        lax.fori_loop(0, 6, chunk, 0)

    def store_b(which, tile):
        cols = pl.ds(pl.multiple_of(tile * w_cols, w_cols), w_cols)
        vals = acc[...]
        soft = jax.nn.sigmoid(vals)

        @pl.when(which < 3)
        def _():
            kvq[which, :, cols] = (vals * soft).astype(BF16)

        @pl.when(which == 3)
        def _():
            gate[:, cols] = soft

    def query_slot(batch):
        return jnp.where(batch == 3, 2, lax.rem(batch, 2))

    def store_a(batch, j):
        @pl.when((j >= kv_tiles) & (j < 2 * kv_tiles))
        def _():
            cols = pl.ds(pl.multiple_of(j * w_cols, w_cols), w_cols)
            kv_own[:, cols] = acc[...].astype(BF16)

        @pl.when((j < kv_tiles) | (j >= 2 * kv_tiles))
        def _():
            for e in range(w_cols // HEAD):
                raw = acc[:, e * HEAD : (e + 1) * HEAD]
                turned = raw * rope[0] + pltpu.roll(raw, HEAD - HEAD // 4, 1) * rope[1]
                turned = (turned + pltpu.roll(raw, HEAD // 4, 1) * rope[2]).astype(BF16)

                @pl.when(j < kv_tiles)
                def _():
                    kv_own[:, pl.ds(pl.multiple_of(j * w_cols + e * HEAD, HEAD), HEAD)] = turned

                @pl.when(j >= 2 * kv_tiles)
                def _():
                    cols = pl.ds(pl.multiple_of((j - 2 * kv_tiles) * w_cols + e * HEAD, HEAD), HEAD)
                    kvq[query_slot(batch), :, cols] = turned

        @pl.when(j == 2 * kv_tiles - 1)
        def _():
            kv_store(batch).start()
            for k in range(1, n_cp):

                @pl.when(c + k < n_cp)
                def _():
                    kv_copy(batch, k).start()

    def kv_store(batch):
        return pltpu.make_async_copy(kv_own, kv_all.at[batch, c], kv_load.at[n_cp])

    def kv_copy(batch, k):
        return pltpu.make_async_remote_copy(
            src_ref=kv_own,
            dst_ref=kv_all.at[batch, c],
            send_sem=kv_send.at[k],
            recv_sem=kv_recv.at[batch, c],
            device_id={"cp": c + k},
            device_id_type=MESH,
        )

    def kv_arrival(batch, source):
        return pltpu.make_async_remote_copy(
            src_ref=kv_own,
            dst_ref=kv_all.at[batch, source],
            send_sem=kv_send.at[0],
            recv_sem=kv_recv.at[batch, source],
            device_id={"cp": source},
            device_id_type=MESH,
        )

    def kv_fetch(batch, source):
        return pltpu.make_async_copy(kv_all.at[batch, source], kv_buf.at[source], kv_load.at[source])

    def load_kv(batch):
        kv_store(batch).wait()
        for k in range(1, n_cp):

            @pl.when(c + k < n_cp)
            def _():
                kv_copy(batch, k).wait_send()

        for source in range(n_cp):

            @pl.when(source < c)
            def _():
                kv_arrival(batch, source).wait_recv()

            @pl.when(source <= c)
            def _():
                kv_fetch(batch, source).start()

        for source in range(n_cp):

            @pl.when(source <= c)
            def _():
                kv_fetch(batch, source).wait()

    def attend(batch, pair):
        kv_head = lax.div(2 * pair, group)
        key_cols = pl.ds(pl.multiple_of(kv_head * HEAD, HEAD), HEAD)
        value_cols = pl.ds(pl.multiple_of(kv_width + kv_head * HEAD, HEAD), HEAD)
        head_cols = [pl.ds(pl.multiple_of((2 * pair + e) * HEAD, HEAD), HEAD) for e in range(2)]
        at = query_slot(batch)
        score_refs = (o_buf, gate)
        top_refs = (sq_acc, row_inv)
        power = math.log2(math.e) / math.sqrt(HEAD)

        def span(j):
            return pl.ds(pl.multiple_of(j * n_tok, n_tok), n_tok)

        rows_at = lax.broadcasted_iota(jnp.int32, (n_tok, n_tok), 0)
        keys_at = lax.broadcasted_iota(jnp.int32, (n_tok, n_tok), 1)
        for e in range(2):
            scores = dot_t(kvq[at, :, head_cols[e]], kv_buf[c, :, key_cols])
            scores = jnp.where(rows_at >= keys_at, scores, -jnp.inf)
            score_refs[e][:, span(c)] = scores
            top_refs[e][...] = fold(scores, jnp.maximum, jnp.max, 1.0)

        def score(j, carry):
            for e in range(2):
                scores = dot_t(kvq[at, :, head_cols[e]], kv_buf[j, :, key_cols])
                score_refs[e][:, span(j)] = scores
                top_refs[e][...] = jnp.maximum(top_refs[e][...], fold(scores, jnp.maximum, jnp.max, 1.0))
            return carry

        lax.fori_loop(0, c, score, 0)
        for e in range(2):
            top_refs[e][...] = jnp.broadcast_to(jnp.max(top_refs[e][...], axis=-1, keepdims=True), (n_tok, HEAD))
            sums[e] = jnp.zeros((n_tok, HEAD), F32)
            acc[:, e * HEAD : (e + 1) * HEAD] = jnp.zeros((n_tok, HEAD), F32)

        def weigh(j, carry):
            for e in range(2):
                probs = jnp.exp2((score_refs[e][:, span(j)] - top_refs[e][:, 0:1]) * power)
                sums[e] += fold(probs, jnp.add, jnp.sum, 1.0 / HEAD)
                acc[:, e * HEAD : (e + 1) * HEAD] += dot(probs.astype(BF16), kv_buf[j, :, value_cols])
            return carry

        lax.fori_loop(0, c + 1, weigh, 0)
        for e in range(2):
            total = jnp.sum(sums[e], axis=-1, keepdims=True)
            y_buf[:, head_cols[e]] = (acc[:, e * HEAD : (e + 1) * HEAD] / total).astype(BF16)

    def out_project(phase, tile):
        wo_copy(wo_a, tile).wait()
        slot = lax.rem(tile, 2)
        cols = pl.ds(pl.multiple_of(tile * wo_cols, wo_cols), wo_cols)
        at = lax.rem(phase + 1, 2)
        part[at, :, cols] = dot(y_buf[...], wo_buf[slot]).astype(BF16)

    def state_copy():
        return pltpu.make_async_remote_copy(
            src_ref=state,
            dst_ref=state_in,
            send_sem=state_send,
            recv_sem=state_recv,
            device_id={"cp": c + 1},
            device_id_type=MESH,
        )

    def local_lightning():
        def head(h, carry):
            cols = pl.ds(pl.multiple_of(h * HEAD, HEAD), HEAD)
            rate = slopes[h]
            key, value, query = kvq[0, :, cols], kvq[1, :, cols], kvq[2, :, cols]
            scores = dot_t(query, key)
            gap = lax.broadcasted_iota(jnp.int32, scores.shape, 0) - lax.broadcasted_iota(jnp.int32, scores.shape, 1)
            decay = jnp.where(gap >= 0, jnp.exp(-rate * gap.astype(F32)), 0.0)
            o_buf[:, cols] = dot((scores * decay).astype(BF16), value)
            to_end = (n_tok - 1 - lax.broadcasted_iota(jnp.int32, (n_tok, HEAD), 0)).astype(F32)
            faded = key.astype(F32) * jnp.exp(-rate * to_end)
            state[h] = dot(faded.T.astype(BF16), value)
            return carry

        lax.fori_loop(0, n_heads, head, 0)

    def add_incoming():
        def head(h, carry):
            state[h] = state_in[h] * jnp.exp(jnp.zeros((HEAD, HEAD), F32) - slopes[h] * n_tok) + state[h]
            return carry

        lax.fori_loop(0, n_heads, head, 0)

    def send_state(batch):
        @pl.when(batch > 0)
        def _():
            pl.semaphore_wait(credit, 1)

        state_copy().start()

    def sq_copy(batch, k):
        peer = lax.rem(z + k, n_tp)
        return pltpu.make_async_remote_copy(
            src_ref=sq_send,
            dst_ref=sq_recv.at[batch, z],
            send_sem=sq_send_sem.at[k],
            recv_sem=sq_recv_sem.at[batch, z],
            device_id={"tp": peer},
            device_id_type=MESH,
        )

    def sq_arrival(batch, k):
        source = lax.rem(z + n_tp - k, n_tp)
        return pltpu.make_async_remote_copy(
            src_ref=sq_send,
            dst_ref=sq_recv.at[batch, source],
            send_sem=sq_send_sem.at[k],
            recv_sem=sq_recv_sem.at[batch, source],
            device_id={"tp": source},
            device_id_type=MESH,
        )

    def add_earlier(batch):
        @pl.when(c == n_cp - 1)
        def _():
            state_copy().wait_recv()

        @pl.when(c < n_cp - 1)
        def _():
            state_copy().wait_send()

        sq_acc[...] = jnp.zeros_like(sq_acc)

        def head(h, carry):
            cols = pl.ds(pl.multiple_of(h * HEAD, HEAD), HEAD)

            @pl.when(c > 0)
            def _():
                steps = (lax.broadcasted_iota(jnp.int32, (n_tok, HEAD), 0) + 1).astype(F32)
                prior = dot(kvq[2, :, cols], state_in[h].astype(BF16))
                o_buf[:, cols] += prior * jnp.exp(-slopes[h] * steps)

            vals = o_buf[:, cols]
            sq_acc[...] += vals * vals
            return carry

        lax.fori_loop(0, n_heads, head, 0)

        @pl.when((c > 0) & (batch < n_batch - 1))
        def _():
            pl.semaphore_signal(credit, inc=1, device_id={"cp": c - 1}, device_id_type=MESH)

        row_sq = jnp.broadcast_to(jnp.sum(sq_acc[...], axis=-1, keepdims=True), (n_tok, HEAD))
        sq_send[...] = row_sq.T[0:8, :]
        sq_recv[batch, z] = sq_send[...]
        for k in range(1, n_tp):
            sq_copy(batch, k).start()

    def finish_lightning(batch):
        for k in range(1, n_tp):
            sq_arrival(batch, k).wait_recv()
        for k in range(1, n_tp):
            sq_copy(batch, k).wait_send()
        total = sq_recv[batch, 0]
        for k in range(1, n_tp):
            total = total + sq_recv[batch, k]
        tall = jnp.broadcast_to(total[0:1, :], (HEAD, n_tok)).T
        row_inv[...] = lax.rsqrt(tall / (width * n_tp) + NORM_EPS)

        def head(h, carry):
            cols = pl.ds(pl.multiple_of(h * HEAD, HEAD), HEAD)
            y_buf[:, cols] = (o_buf[:, cols] * row_inv[...] * ginner[h] * gate[:, cols]).astype(BF16)
            return carry

        lax.fori_loop(0, n_heads, head, 0)

    def unit_body(unit, carry):
        phase = lax.div(unit, UNITS) - 1
        r = lax.rem(unit, UNITS)
        which = lax.div(r, 8)
        tile = lax.rem(r, 8)
        first_layer = phase < n_batch - 1
        second_layer = (phase >= 3) & (phase < 3 + n_batch)
        projects = has_projection(phase)

        @pl.when(lax.rem(tile, 3) == 0)
        def _():
            part_of = lax.div(tile, 3)

            def one(i, inner):
                service(phase * per_batch + which * per_group + part_of * (per_group // 3) + i)
                return inner

            if per_group == 3:
                one(0, 0)
            else:
                lax.fori_loop(0, per_group // 3, one, 0)

        for at_phase, at_r, batch in ((0, 0, 1), (0, 12, 2), (1, 0, 3)):

            @pl.when((phase == at_phase) & (r == at_r))
            def _():
                hidden_copy(batch).wait()

        for at_phase, batch in ((-1, 2), (0, 3)):

            @pl.when((phase == at_phase) & (r == 12))
            def _():
                hidden_copy(batch).start()

        @pl.when(first_layer & (r == jnp.where(phase <= 0, 12, 0)))
        def _():
            load_kv(phase + 1)

        early = phase <= 0
        spread = 16 // n_pairs
        first_pair = jnp.where(early, (r - 12) * (n_pairs // 4), lax.div(r, spread))
        n_here = jnp.where(early, jnp.where(r >= 12, n_pairs // 4, 0), jnp.where(lax.rem(r, spread) == 0, 1, 0))

        @pl.when(first_layer & (r < 16))
        def _():
            def one_pair(i, inner):
                attend(phase + 1, first_pair + i)
                return inner

            lax.fori_loop(0, n_here, one_pair, 0)

        for i in range(2):

            @pl.when((r == 8 + i) & first_layer)
            def _():
                wo_copy(wo_a, i).start()

            @pl.when((r == 8 + i) & second_layer)
            def _():
                wo_copy(wo_l, i).start()

        @pl.when((r == 4) & second_layer & (c == 2))
        def _():
            state_copy().wait_recv()
            add_incoming()
            send_state(phase - 3)

        @pl.when((r == 12) & second_layer)
        def _():
            add_earlier(phase - 3)

        @pl.when((r == 16) & second_layer)
        def _():
            finish_lightning(phase - 3)

        wo_tile = r - 16

        @pl.when((wo_tile >= 0) & (wo_tile < n_wo) & (first_layer | second_layer))
        def _():
            out_project(phase, wo_tile)

            @pl.when((wo_tile < n_wo - 2) & first_layer)
            def _():
                wo_copy(wo_a, wo_tile + 2).start()

            @pl.when((wo_tile < n_wo - 2) & second_layer)
            def _():
                wo_copy(wo_l, wo_tile + 2).start()

        is_a, a_batch, a_j = a_tile(unit)

        @pl.when(is_a | projects)
        def _():
            project(unit, jnp.where(is_a, lax.rem(a_batch, 2), lax.rem(phase, 2)))

            @pl.when(is_a)
            def _():
                store_a(a_batch, a_j)

            @pl.when(projects)
            def _():
                store_b(which, tile)

        fetch(unit + W_SLOTS)

        @pl.when((r == 23) & projects)
        def _():
            local_lightning()

            @pl.when(c == 0)
            def _():
                send_state(phase - 2)

        @pl.when((r == 28) & projects & (c == 1))
        def _():
            state_copy().wait_recv()
            add_incoming()
            send_state(phase - 2)

        return carry

    hidden_copy(0).wait()
    n_phases = 2 * n_batch + 2
    lax.fori_loop(0, n_phases * UNITS, unit_body, 0)
    for f in range(2):
        for k in range(4):
            out_copy(pieces - 4 + k, f, out).wait()


def copy_kernel(src, dst):
    dst[...] = src[...]


def plain_copy(array, blocks):
    n_rows, n_cols = array.shape
    spec = pl.BlockSpec((n_rows // blocks, n_cols), lambda i: (i, 0))
    return pl.pallas_call(copy_kernel, out_shape=jax.ShapeDtypeStruct(array.shape, array.dtype), grid=(blocks,), in_specs=[spec], out_specs=spec)(array)


def fused_layers(hid, weights, gains, ginner, alphas, slopes, n_tok, n_tp, n_cp):
    n_rows, model = hid.shape
    width = weights[2].shape[1]
    kv_width = weights[0].shape[1]
    n_batch = n_rows // n_tok
    n_heads = width // HEAD
    rows = n_tok // 24
    w_cols = width // 8
    wo_cols = model // 12
    vmem, dma = pltpu.VMEM, pltpu.SemaphoreType.DMA
    scratch = [
        vmem((2, n_tok, model), BF16),
        vmem((2, n_tok, model), BF16),
        vmem((2, n_tok, model), BF16),
        vmem((W_SLOTS, model, w_cols), BF16),
        vmem((2, width, wo_cols), BF16),
        vmem((n_tok, width), BF16),
        vmem((3, n_tok, width), BF16),
        vmem((n_tok, width), F32),
        vmem((n_tok, width), F32),
        vmem((n_heads, HEAD, HEAD), F32),
        vmem((n_heads, HEAD, HEAD), F32),
        vmem((2, 4, rows, model), BF16),
        vmem((rows, model), F32),
        vmem((n_tok, w_cols), F32),
        vmem((n_tok, HEAD), F32),
        vmem((n_tok, HEAD), F32),
        vmem((8, n_tok), F32),
        vmem((n_batch, n_tp, 8, n_tok), F32),
        vmem((n_tok, 2 * kv_width), BF16),
        vmem((n_cp, n_tok, 2 * kv_width), BF16),
        vmem((3, n_tok, HEAD), F32),
        vmem((2, n_tok, HEAD), F32),
        dma((2, RING)),
        dma((2, RING)),
        dma((2, RING)),
        dma((2, RING)),
        dma((2, 4)),
        dma((2, 4)),
        dma((W_SLOTS,)),
        dma((2,)),
        dma((2,)),
        dma,
        dma((n_cp,)),
        dma((n_batch, n_cp)),
        dma((n_cp + 1,)),
        dma,
        dma,
        dma((n_tp,)),
        dma((n_batch, n_tp)),
        pltpu.SemaphoreType.REGULAR,
    ]
    flops = 2 * n_rows * model * width * 8
    return pl.pallas_call(
        functools.partial(fused_kernel, n_tp, n_cp),
        out_shape=[
            jax.ShapeDtypeStruct((n_rows, model), BF16),
            jax.ShapeDtypeStruct((n_rows, model), BF16),
            jax.ShapeDtypeStruct((n_batch, n_cp, n_tok, 2 * kv_width), BF16),
        ],
        in_specs=[ANY] * 11 + [VMEM] * 2 + [SMEM] * 2,
        out_specs=[ANY] * 3,
        scratch_shapes=scratch,
        compiler_params=pltpu.CompilerParams(collective_id=0, has_side_effects=True, vmem_limit_bytes=67043328),
        cost_estimate=pl.CostEstimate(flops=flops, bytes_accessed=12 * n_rows * model, transcendentals=0),
    )(hid, *weights, rotary_table(n_tok * n_cp), gains, ginner, alphas, slopes)


def solution(mesh):
    n_tp, n_cp = mesh.shape["tp"], mesh.shape["cp"]

    def body(hidden, alphas, wq_attn, wk_attn, wv_attn, wo_attn, gain_attn, wq_lin, wk_lin, wv_lin, wg_lin, slopes, gain_inner, wo_lin, gain_lin):
        n_batch, n_tok, model = hidden.shape
        flat = hidden.reshape(n_batch * n_tok, model)
        gains = jnp.stack([gain_attn, gain_lin])[:, None, :]
        weights = (wk_attn, wv_attn, wq_attn, wo_attn, wk_lin, wv_lin, wq_lin, wg_lin, wo_lin)
        outs = fused_layers(flat, weights, gains, gain_inner.reshape(-1, 1, HEAD), alphas, slopes, n_tok, n_tp, n_cp)
        return plain_copy(outs[0], 12).reshape(hidden.shape)

    act_spec = P("dp", "cp", None)
    rep_spec = P()
    col_spec = P(None, "tp")
    row_spec = P("tp", None)
    vec_spec = P("tp")
    in_specs = (act_spec, rep_spec, col_spec, col_spec, col_spec, row_spec, rep_spec, col_spec, col_spec, col_spec, col_spec, vec_spec, vec_spec, row_spec, rep_spec)
    return jax.shard_map(body, mesh=mesh, in_specs=in_specs, out_specs=act_spec, check_vma=False)
```

```python
import functools
import math

import jax
import jax.numpy as jnp
import numpy as np
from jax import lax
from jax.experimental import pallas as pl
from jax.experimental.pallas import tpu as pltpu
from jax.sharding import PartitionSpec as P

ROPE_BASE = 10000000.0
NORM_EPS = 1e-5
HEAD = 128
MESH = pl.DeviceIdType.MESH
F32 = jnp.float32
BF16 = jnp.bfloat16
ANY = pl.BlockSpec(memory_space=pl.ANY)
VMEM = pl.BlockSpec(memory_space=pltpu.VMEM)
SMEM = pl.BlockSpec(memory_space=pltpu.SMEM)

LEAD = 2
RING = 16
UNITS = 32
W_SLOTS = 3


def dot(lhs, rhs):
    return jnp.dot(lhs, rhs, preferred_element_type=F32)


def dot_t(lhs, rhs):
    return lax.dot_general(lhs, rhs, (((1,), (1,)), ((), ())), preferred_element_type=F32)


def rotary_table(n_pos):
    half = HEAD // 4
    inv_freq = np.power(ROPE_BASE, -np.arange(half) * 2.0 / (2 * half)).astype(np.float32)
    angles = (np.arange(n_pos, dtype=np.float32)[:, None] * inv_freq[None, :]).astype(np.float64)
    cosine, sine = np.cos(angles), np.sin(angles)
    return np.concatenate([cosine, cosine, sine, sine], axis=1).astype(np.float32)


def fold(vals, op, reduce, share):
    n_cols = vals.shape[1]
    if n_cols % HEAD:
        return jnp.broadcast_to(reduce(vals, axis=-1, keepdims=True) * share, (vals.shape[0], HEAD))
    out = vals[:, 0:HEAD]
    for k in range(1, n_cols // HEAD):
        out = op(out, vals[:, k * HEAD : (k + 1) * HEAD])
    return out


def fused_kernel(
    n_tp,
    n_cp,
    hid,
    wk_a,
    wv_a,
    wq_a,
    wo_a,
    wk,
    wv,
    wq,
    wg,
    wo_l,
    table,
    gain_a,
    gain_l,
    ginner,
    alphas,
    slopes,
    out,
    h1,
    kv_all,
    part,
    summed,
    normed,
    w_buf,
    wo_buf,
    y_buf,
    kvq,
    gate,
    o_buf,
    state,
    state_in,
    res,
    wide,
    gains,
    acc,
    sq_acc,
    row_inv,
    sq_send,
    sq_recv,
    kv_own,
    kv_buf,
    rope,
    sums,
    reduce_send,
    reduce_recv,
    back_send,
    back_recv,
    res_sem,
    out_sem,
    w_sem,
    wo_sem,
    hid_sem,
    rope_sem,
    kv_send,
    kv_recv,
    kv_load,
    state_send,
    state_recv,
    sq_send_sem,
    sq_recv_sem,
    credit,
):
    _, n_tok, model = part.shape
    width = y_buf.shape[1]
    n_heads = width // HEAD
    n_batch = hid.shape[0] // n_tok
    kv_width = wk_a.shape[1]
    group = width // kv_width
    half = n_tok // 2
    rows = res.shape[2]
    per_batch = half // rows
    per_group = per_batch // 4
    layer_pieces = n_batch * per_batch
    pieces = 2 * layer_pieces
    w_cols = w_buf.shape[2]
    wo_cols = wo_buf.shape[2]
    n_wo = model // wo_cols
    kv_tiles = kv_width // w_cols
    a_tiles = 2 * kv_tiles + 8
    last = n_tp - 1
    trip = 2 * last * LEAD
    z = lax.axis_index("tp")
    c = lax.axis_index("cp")

    def hidden_copy(batch):
        at = lax.rem(batch, 2)
        return pltpu.make_async_copy(hid.at[pl.ds(pl.multiple_of(batch * n_tok, n_tok), n_tok), :], normed.at[at], hid_sem.at[at])

    def a_tile(unit):
        phase = lax.div(unit, UNITS) - 1
        r = lax.rem(unit, UNITS)
        late = r >= 20
        j = jnp.where(late, r - 20, r)
        is_a = (phase <= 1) & (j < a_tiles) & (jnp.logical_not(late) | (phase == 0))
        batch = jnp.where(phase == 1, 3, jnp.where(late, 2, phase + 1))
        return is_a, batch, j

    def w_cut(weight, tile, slot):
        cols = pl.ds(pl.multiple_of(tile * w_cols, w_cols), w_cols)
        return pltpu.make_async_copy(weight.at[:, cols], w_buf.at[slot], w_sem.at[slot])

    def fetch(unit):
        slot = lax.rem(unit, W_SLOTS)
        r = lax.rem(unit, UNITS)
        phase = lax.div(unit, UNITS) - 1

        @pl.when(phase <= 1)
        def _():
            is_a, _, j = a_tile(unit)

            @pl.when(is_a & (j >= 2 * kv_tiles))
            def _():
                w_cut(wq_a, j - 2 * kv_tiles, slot).start()

            @pl.when(is_a & (j < 2 * kv_tiles))
            def _():
                @pl.when(j < kv_tiles)
                def _():
                    w_cut(wk_a, j, slot).start()

                @pl.when(j >= kv_tiles)
                def _():
                    w_cut(wv_a, j - kv_tiles, slot).start()

        @pl.when(has_projection(phase))
        def _():
            for k, weight in enumerate((wk, wv, wq, wg)):

                @pl.when(lax.div(r, 8) == k)
                def _():
                    w_cut(weight, lax.rem(r, 8), slot).start()

    def has_projection(phase):
        return (phase >= 2) & (phase < 2 + n_batch)

    for i in range(2):
        hidden_copy(i).start()
    for i in range(W_SLOTS):
        fetch(jnp.int32(i))
    table_copy = pltpu.make_async_copy(table.at[pl.ds(pl.multiple_of(c * n_tok, n_tok), n_tok), :], rope.at[0], rope_sem)
    table_copy.start()

    barrier = pltpu.get_barrier_semaphore()
    for k in range(1, n_tp):
        pl.semaphore_signal(barrier, inc=1, device_id={"tp": lax.rem(z + k, n_tp)}, device_id_type=MESH)
    for k in range(1, n_cp):
        pl.semaphore_signal(barrier, inc=1, device_id={"cp": lax.rem(c + k, n_cp)}, device_id_type=MESH)

    gains[0] = gain_a[...]
    gains[1] = gain_l[...]
    table_copy.wait()
    lane = lax.broadcasted_iota(jnp.int32, (n_tok, HEAD), 1)
    cosines = rope[0]
    sines = pltpu.roll(cosines, HEAD // 2, 1)
    rope[0] = jnp.where(lane < HEAD // 2, cosines, 1.0)
    rope[1] = jnp.where(lane < HEAD // 4, -sines, 0.0)
    rope[2] = jnp.where((lane >= HEAD // 4) & (lane < HEAD // 2), sines, 0.0)
    pl.semaphore_wait(barrier, n_tp + n_cp - 2)

    def row_of(g, f):
        return pl.multiple_of(f * half + lax.rem(g, per_batch) * rows, rows)

    def view(ref, g, f):
        return ref.at[lax.rem(lax.div(g, per_batch), 2), pl.ds(row_of(g, f), rows), :]

    def place(f):
        return (z, z + 1, z - 1) if f == 0 else (last - z, z - 1, z + 1)

    def forward(g, f):
        slot = lax.rem(g, RING)
        return pltpu.make_async_remote_copy(
            src_ref=view(part, g, f),
            dst_ref=view(summed, g, f),
            send_sem=reduce_send.at[f, slot],
            recv_sem=reduce_recv.at[f, slot],
            device_id={"tp": place(f)[1]},
            device_id_type=MESH,
        )

    def backward(g, f):
        slot = lax.rem(g, RING)
        return pltpu.make_async_remote_copy(
            src_ref=view(summed, g, f),
            dst_ref=view(summed, g, f),
            send_sem=back_send.at[f, slot],
            recv_sem=back_recv.at[f, slot],
            device_id={"tp": place(f)[2]},
            device_id_type=MESH,
        )

    def hbm_rows(ref, g, f):
        batch = lax.rem(lax.div(g, per_batch), n_batch)
        return ref.at[pl.ds(pl.multiple_of(batch * n_tok + row_of(g, f), rows), rows), :]

    def res_copy(g, f, ref):
        slot = lax.rem(g, 4)
        return pltpu.make_async_copy(hbm_rows(ref, g, f), res.at[f, slot], res_sem.at[f, slot])

    def out_copy(g, f, ref):
        return pltpu.make_async_copy(view(normed, g, f), hbm_rows(ref, g, f), out_sem.at[f, lax.rem(g, 4)])

    def norm_rows(g):
        layer = (g >= layer_pieces).astype(jnp.int32)
        slot = lax.rem(g, 4)
        at = lax.rem(lax.div(g, per_batch), 2)
        alpha = alphas[layer]
        chunks = [slice(i * wo_cols, (i + 1) * wo_cols) for i in range(n_wo)]
        for f in range(2):
            span = pl.ds(row_of(g, f), rows)
            sq = jnp.zeros((rows, wo_cols), F32)
            for cols in chunks:
                vals = alpha * res[f, slot, :, cols].astype(F32) + summed[at, span, cols].astype(F32)
                wide[f, :, cols] = vals
                sq = sq + vals * vals
            scale = lax.rsqrt(jnp.sum(sq, axis=-1, keepdims=True) / model + NORM_EPS)
            for cols in chunks:
                normed[at, span, cols] = (wide[f, :, cols] * scale * gains[layer, :, cols]).astype(BF16)

    def known(g):
        return (g >= 0) & (g < pieces)

    def service(step):
        ahead = step + 3 - trip
        for f in range(2):

            @pl.when((ahead >= 0) & (ahead < layer_pieces))
            def _():
                res_copy(ahead, f, hid).start()

            @pl.when((ahead >= layer_pieces) & (ahead < pieces))
            def _():
                res_copy(ahead, f, h1).start()

        for f in range(2):
            pos = place(f)[0]
            g = step - LEAD * pos

            @pl.when(known(g) & (pos > 0))
            def _():
                forward(g, f).wait_recv()

            @pl.when(known(g) & (pos > 0) & (pos < last))
            def _():
                at = lax.rem(lax.div(g, per_batch), 2)
                span = pl.ds(row_of(g, f), rows)
                part[at, span, :] = part[at, span, :] + summed[at, span, :]

            @pl.when(known(g) & (pos == last))
            def _():
                at = lax.rem(lax.div(g, per_batch), 2)
                span = pl.ds(row_of(g, f), rows)
                summed[at, span, :] = part[at, span, :] + summed[at, span, :]

        for f in range(2):
            pos = place(f)[0]
            g = step - LEAD * pos

            @pl.when(known(g) & (pos < last))
            def _():
                forward(g, f).start()

            @pl.when(known(g) & (pos == last))
            def _():
                backward(g, f).start()

        for f in range(2):
            pos = place(f)[0]
            g = step - LEAD * (2 * last - pos)

            @pl.when(known(g) & (pos < last))
            def _():
                backward(g, f).wait_recv()

            @pl.when(known(g) & (pos < last) & (pos > 0))
            def _():
                backward(g, f).start()

        for f in range(2):
            pos = place(f)[0]
            sent = step - (LEAD * (last - 1) + 3)

            @pl.when(known(sent) & (pos < last))
            def _():
                forward(sent, f).wait_send()

        done = step - trip

        @pl.when(known(done))
        def _():
            for f in range(2):
                pos = place(f)[0]

                @pl.when(pos > 0)
                def _():
                    backward(done, f).wait_send()

                res_copy(done, f, hid).wait()

                @pl.when(done >= 4)
                def _():
                    out_copy(done - 4, f, out).wait()

            norm_rows(done)

            @pl.when(done < layer_pieces)
            def _():
                for f in range(2):
                    out_copy(done, f, h1).start()

            @pl.when(done >= layer_pieces)
            def _():
                for f in range(2):
                    out_copy(done, f, out).start()

    def wo_copy(weight, tile):
        cols = pl.ds(pl.multiple_of(tile * wo_cols, wo_cols), wo_cols)
        slot = lax.rem(tile, 2)
        return pltpu.make_async_copy(weight.at[:, cols], wo_buf.at[slot], wo_sem.at[slot])

    halves = (slice(0, half), slice(half, n_tok))

    def project_a(unit, batch, j):
        slot = lax.rem(unit, W_SLOTS)
        at = lax.rem(batch, 2)
        w_cut(wk, 0, slot).wait()
        for span in halves:
            acc[span, :] = dot(normed[at, span, :], w_buf[slot])
        store_a(batch, j)

    def project_b(unit, at, which, tile):
        slot = lax.rem(unit, W_SLOTS)
        w_cut(wk, 0, slot).wait()
        cols = pl.ds(pl.multiple_of(tile * w_cols, w_cols), w_cols)

        @pl.when(which < 3)
        def _():
            for span in halves:
                vals = dot(normed[at, span, :], w_buf[slot])
                kvq[which, span, cols] = (vals * jax.nn.sigmoid(vals)).astype(BF16)

        @pl.when(which == 3)
        def _():
            for span in halves:
                gate[span, cols] = jax.nn.sigmoid(dot(normed[at, span, :], w_buf[slot]))

    def query_slot(batch):
        return jnp.where(batch == 3, 2, lax.rem(batch, 2))

    def store_a(batch, j):
        @pl.when((j >= kv_tiles) & (j < 2 * kv_tiles))
        def _():
            cols = pl.ds(pl.multiple_of(j * w_cols, w_cols), w_cols)
            kv_own[:, cols] = acc[...].astype(BF16)

        @pl.when((j < kv_tiles) | (j >= 2 * kv_tiles))
        def _():
            for e in range(w_cols // HEAD):
                raw = acc[:, e * HEAD : (e + 1) * HEAD]
                turned = raw * rope[0] + pltpu.roll(raw, HEAD - HEAD // 4, 1) * rope[1]
                turned = (turned + pltpu.roll(raw, HEAD // 4, 1) * rope[2]).astype(BF16)

                @pl.when(j < kv_tiles)
                def _():
                    kv_own[:, pl.ds(pl.multiple_of(j * w_cols + e * HEAD, HEAD), HEAD)] = turned

                @pl.when(j >= 2 * kv_tiles)
                def _():
                    cols = pl.ds(pl.multiple_of((j - 2 * kv_tiles) * w_cols + e * HEAD, HEAD), HEAD)
                    kvq[query_slot(batch), :, cols] = turned

        @pl.when(j == 2 * kv_tiles - 1)
        def _():
            kv_store(batch).start()
            for mine, theirs in kv_routes:

                @pl.when(c == mine)
                def _():
                    kv_copy(batch, theirs).start()

    def kv_store(batch):
        return pltpu.make_async_copy(kv_own, kv_all.at[batch, c], kv_load.at[n_cp])

    kv_routes = ((0, 1), (0, 2), (1, 3), (2, 3))
    kv_relays = ((2, 0, 3), (3, 1, 2))

    def kv_copy(batch, to):
        return pltpu.make_async_remote_copy(
            src_ref=kv_own,
            dst_ref=kv_all.at[batch, c],
            send_sem=kv_send.at[to],
            recv_sem=kv_recv.at[batch, c],
            device_id={"cp": to},
            device_id_type=MESH,
        )

    def kv_relay(batch, source, to):
        return pltpu.make_async_remote_copy(
            src_ref=kv_all.at[batch, source],
            dst_ref=kv_all.at[batch, source],
            send_sem=kv_send.at[to],
            recv_sem=kv_recv.at[batch, source],
            device_id={"cp": to},
            device_id_type=MESH,
        )

    def kv_fetch(batch, source):
        return pltpu.make_async_copy(kv_all.at[batch, source], kv_buf.at[source], kv_load.at[source])

    def load_kv(batch):
        kv_store(batch).wait()
        for mine, theirs in kv_routes:

            @pl.when(c == mine)
            def _():
                kv_copy(batch, theirs).wait_send()

        for mine, source, theirs in kv_relays:

            @pl.when(c == mine)
            def _():
                kv_relay(batch, source, theirs).wait_recv()
                kv_relay(batch, source, theirs).start()

        for source in range(n_cp):

            @pl.when((source < c) & ((c < 2) | (source != c - 2)))
            def _():
                kv_relay(batch, source, source).wait_recv()

            @pl.when(source <= c)
            def _():
                kv_fetch(batch, source).start()

        for source in range(n_cp):

            @pl.when(source <= c)
            def _():
                kv_fetch(batch, source).wait()

        for mine, source, theirs in kv_relays:

            @pl.when(c == mine)
            def _():
                kv_relay(batch, source, theirs).wait_send()

    def attend(batch, pair):
        kv_head = lax.div(2 * pair, group)
        key_cols = pl.ds(pl.multiple_of(kv_head * HEAD, HEAD), HEAD)
        value_cols = pl.ds(pl.multiple_of(kv_width + kv_head * HEAD, HEAD), HEAD)
        head_cols = [pl.ds(pl.multiple_of((2 * pair + e) * HEAD, HEAD), HEAD) for e in range(2)]
        at = query_slot(batch)
        score_refs = (o_buf, gate)
        top_refs = (sq_acc, row_inv)
        power = math.log2(math.e) / math.sqrt(HEAD)

        def span(j):
            return pl.ds(pl.multiple_of(j * n_tok, n_tok), n_tok)

        rows_at = lax.broadcasted_iota(jnp.int32, (n_tok, n_tok), 0)
        keys_at = lax.broadcasted_iota(jnp.int32, (n_tok, n_tok), 1)
        for e in range(2):
            scores = dot_t(kvq[at, :, head_cols[e]], kv_buf[c, :, key_cols])
            scores = jnp.where(rows_at >= keys_at, scores, -jnp.inf)
            score_refs[e][:, span(c)] = scores
            top_refs[e][...] = fold(scores, jnp.maximum, jnp.max, 1.0)

        def score(j, carry):
            for e in range(2):
                scores = dot_t(kvq[at, :, head_cols[e]], kv_buf[j, :, key_cols])
                score_refs[e][:, span(j)] = scores
                top_refs[e][...] = jnp.maximum(top_refs[e][...], fold(scores, jnp.maximum, jnp.max, 1.0))
            return carry

        lax.fori_loop(0, c, score, 0)
        for e in range(2):
            top_refs[e][...] = jnp.broadcast_to(jnp.max(top_refs[e][...], axis=-1, keepdims=True), (n_tok, HEAD))
            sums[e] = jnp.zeros((n_tok, HEAD), F32)
            acc[:, e * HEAD : (e + 1) * HEAD] = jnp.zeros((n_tok, HEAD), F32)

        def weigh(j, carry):
            for e in range(2):
                probs = jnp.exp2((score_refs[e][:, span(j)] - top_refs[e][:, 0:1]) * power)
                sums[e] += fold(probs, jnp.add, jnp.sum, 1.0 / HEAD)
                acc[:, e * HEAD : (e + 1) * HEAD] += dot(probs.astype(BF16), kv_buf[j, :, value_cols])
            return carry

        lax.fori_loop(0, c + 1, weigh, 0)
        for e in range(2):
            total = jnp.sum(sums[e], axis=-1, keepdims=True)
            y_buf[:, head_cols[e]] = (acc[:, e * HEAD : (e + 1) * HEAD] / total).astype(BF16)

    def out_project(phase, tile):
        wo_copy(wo_a, tile).wait()
        slot = lax.rem(tile, 2)
        cols = pl.ds(pl.multiple_of(tile * wo_cols, wo_cols), wo_cols)
        at = lax.rem(phase + 1, 2)
        part[at, :, cols] = dot(y_buf[...], wo_buf[slot]).astype(BF16)

    def state_copy():
        return pltpu.make_async_remote_copy(
            src_ref=state,
            dst_ref=state_in,
            send_sem=state_send,
            recv_sem=state_recv,
            device_id={"cp": c + 1},
            device_id_type=MESH,
        )

    def local_lightning():
        def one_head(h):
            cols = pl.ds(pl.multiple_of(h * HEAD, HEAD), HEAD)
            rate = slopes[h]
            key, value, query = kvq[0, :, cols], kvq[1, :, cols], kvq[2, :, cols]
            part_rows = n_tok // 3
            for i in range(3):
                span = slice(i * part_rows, (i + 1) * part_rows)
                upto = slice(0, (i + 1) * part_rows)
                scores = dot_t(query[span], key[upto])
                gap = lax.broadcasted_iota(jnp.int32, scores.shape, 0) - lax.broadcasted_iota(jnp.int32, scores.shape, 1) + i * part_rows
                decay = jnp.where(gap >= 0, jnp.exp(-rate * gap.astype(F32)), 0.0)
                o_buf[span, cols] = dot((scores * decay).astype(BF16), value[upto])
            to_end = (n_tok - 1 - lax.broadcasted_iota(jnp.int32, (n_tok, HEAD), 0)).astype(F32)
            faded = key.astype(F32) * jnp.exp(-rate * to_end)
            state[h] = dot(faded.T.astype(BF16), value)

        def head_pair(i, carry):
            one_head(2 * i)
            one_head(2 * i + 1)
            return carry

        lax.fori_loop(0, n_heads // 2, head_pair, 0)

    def add_incoming():
        def head(h, carry):
            state[h] = state_in[h] * jnp.exp(jnp.zeros((HEAD, HEAD), F32) - slopes[h] * n_tok) + state[h]
            return carry

        lax.fori_loop(0, n_heads, head, 0)

    def send_state(batch):
        @pl.when(batch > 0)
        def _():
            pl.semaphore_wait(credit, 1)

        state_copy().start()

    def sq_copy(batch, k):
        peer = lax.rem(z + k, n_tp)
        return pltpu.make_async_remote_copy(
            src_ref=sq_send,
            dst_ref=sq_recv.at[batch, z],
            send_sem=sq_send_sem.at[k],
            recv_sem=sq_recv_sem.at[batch, z],
            device_id={"tp": peer},
            device_id_type=MESH,
        )

    def sq_arrival(batch, k):
        source = lax.rem(z + n_tp - k, n_tp)
        return pltpu.make_async_remote_copy(
            src_ref=sq_send,
            dst_ref=sq_recv.at[batch, source],
            send_sem=sq_send_sem.at[k],
            recv_sem=sq_recv_sem.at[batch, source],
            device_id={"tp": source},
            device_id_type=MESH,
        )

    def add_earlier(batch):
        @pl.when(c == n_cp - 1)
        def _():
            state_copy().wait_recv()

        @pl.when(c < n_cp - 1)
        def _():
            state_copy().wait_send()

        sq_acc[...] = jnp.zeros_like(sq_acc)

        def cols_of(h):
            return pl.ds(pl.multiple_of(h * HEAD, HEAD), HEAD)

        def head_pair(i, carry):
            for h in (2 * i, 2 * i + 1):
                steps = (lax.broadcasted_iota(jnp.int32, (n_tok, HEAD), 0) + 1).astype(F32)
                prior = dot(kvq[2, :, cols_of(h)], state_in[h].astype(BF16))
                vals = o_buf[:, cols_of(h)] + prior * jnp.exp(-slopes[h] * steps)
                o_buf[:, cols_of(h)] = vals
                sq_acc[...] += vals * vals
            return carry

        def head(h, carry):
            vals = o_buf[:, cols_of(h)]
            sq_acc[...] += vals * vals
            return carry

        @pl.when(c > 0)
        def _():
            lax.fori_loop(0, n_heads // 2, head_pair, 0)

        @pl.when(c == 0)
        def _():
            lax.fori_loop(0, n_heads, head, 0)

        @pl.when((c > 0) & (batch < n_batch - 1))
        def _():
            pl.semaphore_signal(credit, inc=1, device_id={"cp": c - 1}, device_id_type=MESH)

        row_sq = jnp.broadcast_to(jnp.sum(sq_acc[...], axis=-1, keepdims=True), (n_tok, HEAD))
        sq_send[...] = row_sq.T[0:8, :]
        sq_recv[batch, z] = sq_send[...]
        for k in range(1, n_tp):
            sq_copy(batch, k).start()

    def finish_lightning(batch):
        for k in range(1, n_tp):
            sq_arrival(batch, k).wait_recv()
        for k in range(1, n_tp):
            sq_copy(batch, k).wait_send()
        total = sq_recv[batch, 0]
        for k in range(1, n_tp):
            total = total + sq_recv[batch, k]
        tall = jnp.broadcast_to(total[0:1, :], (HEAD, n_tok)).T
        row_inv[...] = lax.rsqrt(tall / (width * n_tp) + NORM_EPS)

        def head(h, carry):
            cols = pl.ds(pl.multiple_of(h * HEAD, HEAD), HEAD)
            y_buf[:, cols] = (o_buf[:, cols] * row_inv[...] * ginner[h] * gate[:, cols]).astype(BF16)
            return carry

        lax.fori_loop(0, n_heads, head, 0)

    def unit_body(unit, carry):
        phase = lax.div(unit, UNITS) - 1
        r = lax.rem(unit, UNITS)
        which = lax.div(r, 8)
        tile = lax.rem(r, 8)
        first_layer = phase < n_batch - 1
        second_layer = (phase >= 3) & (phase < 3 + n_batch)
        projects = has_projection(phase)

        @pl.when(lax.rem(tile, 3) == 0)
        def _():
            part_of = lax.div(tile, 3)

            def one(i, inner):
                service(phase * per_batch + which * per_group + part_of * (per_group // 3) + i)
                return inner

            if per_group == 3:
                one(0, 0)
            else:
                lax.fori_loop(0, per_group // 3, one, 0)

        @pl.when(lax.rem(r, 4) == 0)
        def _():
            @pl.when(phase <= 2)
            def _():
                for at_phase, at_r, batch in ((0, 0, 1), (0, 20, 2), (1, 0, 3)):

                    @pl.when((phase == at_phase) & (r == at_r))
                    def _():
                        hidden_copy(batch).wait()

                for at_phase, batch in ((-1, 2), (0, 3)):

                    @pl.when((phase == at_phase) & (r == 12))
                    def _():
                        hidden_copy(batch).start()

                @pl.when(r == jnp.where(phase < 0, 12, jnp.where(phase == 0, 8, 0)))
                def _():
                    load_kv(phase + 1)

                @pl.when(r == 8)
                def _():
                    for i in range(2):
                        wo_copy(wo_a, i).start()

            @pl.when(second_layer)
            def _():
                @pl.when((r == 4) & (c == 2))
                def _():
                    state_copy().wait_recv()
                    add_incoming()
                    send_state(phase - 3)

                @pl.when(r == 8)
                def _():
                    for i in range(2):
                        wo_copy(wo_l, i).start()

                @pl.when(r == 12)
                def _():
                    add_earlier(phase - 3)

                @pl.when(r == 16)
                def _():
                    finish_lightning(phase - 3)

            @pl.when(projects)
            def _():
                @pl.when(r == 24)
                def _():
                    local_lightning()

                    @pl.when(c == 0)
                    def _():
                        send_state(phase - 2)

                @pl.when((r == 28) & (c == 1))
                def _():
                    state_copy().wait_recv()
                    add_incoming()
                    send_state(phase - 2)

        @pl.when(first_layer & (r < 16))
        def _():
            later_pair = jnp.where(phase == 0, r - 8, lax.div(r, 2))
            first_pair = jnp.where(phase < 0, (r - 12) * 2, later_pair)
            later_here = jnp.where((phase == 0) & (r >= 8) | (phase > 0) & (lax.rem(r, 2) == 0), 1, 0)
            n_here = jnp.where(phase < 0, jnp.where(r >= 12, 2, 0), later_here)

            def one_pair(i, inner):
                attend(phase + 1, first_pair + i)
                return inner

            lax.fori_loop(0, n_here, one_pair, 0)

        wo_tile = r - 16

        @pl.when((wo_tile >= 0) & (wo_tile < n_wo) & (phase < 3 + n_batch))
        def _():
            out_project(phase, wo_tile)

            @pl.when((wo_tile < n_wo - 2) & first_layer)
            def _():
                wo_copy(wo_a, wo_tile + 2).start()

            @pl.when((wo_tile < n_wo - 2) & second_layer)
            def _():
                wo_copy(wo_l, wo_tile + 2).start()

        @pl.when(phase <= 1)
        def _():
            is_a, a_batch, a_j = a_tile(unit)

            @pl.when(is_a)
            def _():
                project_a(unit, a_batch, a_j)

        @pl.when(projects)
        def _():
            project_b(unit, lax.rem(phase, 2), which, tile)

        fetch(unit + W_SLOTS)
        return carry

    hidden_copy(0).wait()
    n_phases = 2 * n_batch + 2
    lax.fori_loop(0, n_phases * UNITS, unit_body, 0)
    for f in range(2):
        for k in range(4):
            out_copy(pieces - 4 + k, f, out).wait()


def copy_kernel(blocks, src, dst, buf, read_sem, write_sem):
    rows = src.shape[0] // blocks

    def read(i):
        span = pl.ds(i * rows, rows)
        return pltpu.make_async_copy(src.at[span, :], buf.at[span, :], read_sem.at[i])

    def write(i):
        span = pl.ds(i * rows, rows)
        return pltpu.make_async_copy(buf.at[span, :], dst.at[span, :], write_sem.at[i])

    for i in range(blocks):
        read(i).start()
    for i in range(blocks):
        read(i).wait()
        write(i).start()
    for i in range(blocks):
        write(i).wait()


def plain_copy(array, blocks):
    shape = jax.ShapeDtypeStruct(array.shape, array.dtype)
    return pl.pallas_call(
        functools.partial(copy_kernel, blocks),
        out_shape=shape,
        in_specs=[ANY],
        out_specs=ANY,
        scratch_shapes=[pltpu.VMEM(array.shape, array.dtype), pltpu.SemaphoreType.DMA((blocks,)), pltpu.SemaphoreType.DMA((blocks,))],
        compiler_params=pltpu.CompilerParams(vmem_limit_bytes=48 * 1024 * 1024),
    )(array)


def fused_layers(hid, weights, gains, ginner, alphas, slopes, n_tok, n_tp, n_cp):
    n_rows, model = hid.shape
    width = weights[2].shape[1]
    kv_width = weights[0].shape[1]
    n_batch = n_rows // n_tok
    n_heads = width // HEAD
    rows = n_tok // 24
    w_cols = width // 8
    wo_cols = model // 12
    vmem, dma = pltpu.VMEM, pltpu.SemaphoreType.DMA
    scratch = [
        vmem((2, n_tok, model), BF16),
        vmem((2, n_tok, model), BF16),
        vmem((2, n_tok, model), BF16),
        vmem((W_SLOTS, model, w_cols), BF16),
        vmem((2, width, wo_cols), BF16),
        vmem((n_tok, width), BF16),
        vmem((3, n_tok, width), BF16),
        vmem((n_tok, width), F32),
        vmem((n_tok, width), F32),
        vmem((n_heads, HEAD, HEAD), F32),
        vmem((n_heads, HEAD, HEAD), F32),
        vmem((2, 4, rows, model), BF16),
        vmem((2, rows, model), F32),
        vmem((2, 1, model), F32),
        vmem((n_tok, w_cols), F32),
        vmem((n_tok, HEAD), F32),
        vmem((n_tok, HEAD), F32),
        vmem((8, n_tok), F32),
        vmem((n_batch, n_tp, 8, n_tok), F32),
        vmem((n_tok, 2 * kv_width), BF16),
        vmem((n_cp, n_tok, 2 * kv_width), BF16),
        vmem((3, n_tok, HEAD), F32),
        vmem((2, n_tok, HEAD), F32),
        dma((2, RING)),
        dma((2, RING)),
        dma((2, RING)),
        dma((2, RING)),
        dma((2, 4)),
        dma((2, 4)),
        dma((W_SLOTS,)),
        dma((2,)),
        dma((2,)),
        dma,
        dma((n_cp,)),
        dma((n_batch, n_cp)),
        dma((n_cp + 1,)),
        dma,
        dma,
        dma((n_tp,)),
        dma((n_batch, n_tp)),
        pltpu.SemaphoreType.REGULAR,
    ]
    flops = 2 * n_rows * model * width * 8
    return pl.pallas_call(
        functools.partial(fused_kernel, n_tp, n_cp),
        out_shape=[
            jax.ShapeDtypeStruct((n_rows, model), BF16),
            jax.ShapeDtypeStruct((n_rows, model), BF16),
            jax.ShapeDtypeStruct((n_batch, n_cp, n_tok, 2 * kv_width), BF16),
        ],
        in_specs=[ANY] * 11 + [VMEM] * 3 + [SMEM] * 2,
        out_specs=[ANY] * 3,
        scratch_shapes=scratch,
        compiler_params=pltpu.CompilerParams(collective_id=0, has_side_effects=True, vmem_limit_bytes=67043328),
        cost_estimate=pl.CostEstimate(flops=flops, bytes_accessed=12 * n_rows * model, transcendentals=0),
    )(hid, *weights, rotary_table(n_tok * n_cp), *gains, ginner, alphas, slopes)


def solution(mesh):
    n_tp, n_cp = mesh.shape["tp"], mesh.shape["cp"]

    def body(hidden, alphas, wq_attn, wk_attn, wv_attn, wo_attn, gain_attn, wq_lin, wk_lin, wv_lin, wg_lin, slopes, gain_inner, wo_lin, gain_lin):
        n_batch, n_tok, model = hidden.shape
        flat = hidden.reshape(n_batch * n_tok, model)
        gains = (gain_attn[None, :], gain_lin[None, :])
        weights = (wk_attn, wv_attn, wq_attn, wo_attn, wk_lin, wv_lin, wq_lin, wg_lin, wo_lin)
        outs = fused_layers(flat, weights, gains, gain_inner.reshape(-1, 1, HEAD), alphas, slopes, n_tok, n_tp, n_cp)
        return plain_copy(outs[0], 16).reshape(hidden.shape)

    act_spec = P("dp", "cp", None)
    rep_spec = P()
    col_spec = P(None, "tp")
    row_spec = P("tp", None)
    vec_spec = P("tp")
    in_specs = (act_spec, rep_spec, col_spec, col_spec, col_spec, row_spec, rep_spec, col_spec, col_spec, col_spec, col_spec, vec_spec, vec_spec, row_spec, rep_spec)
    return jax.shard_map(body, mesh=mesh, in_specs=in_specs, out_specs=act_spec, check_vma=False)
```

```python
import functools
import math

import jax
import jax.numpy as jnp
import numpy as np
from jax import lax
from jax.experimental import pallas as pl
from jax.experimental.pallas import tpu as pltpu
from jax.sharding import PartitionSpec as P

ROPE_BASE = 10000000.0
NORM_EPS = 1e-5
HEAD = 128
MESH = pl.DeviceIdType.MESH
F32 = jnp.float32
BF16 = jnp.bfloat16
ANY = pl.BlockSpec(memory_space=pl.ANY)
VMEM = pl.BlockSpec(memory_space=pltpu.VMEM)
SMEM = pl.BlockSpec(memory_space=pltpu.SMEM)

LEAD = 2
RING = 16
UNITS = 32
W_SLOTS = 3


def dot(lhs, rhs):
    return jnp.dot(lhs, rhs, preferred_element_type=F32)


def dot_t(lhs, rhs):
    return lax.dot_general(lhs, rhs, (((1,), (1,)), ((), ())), preferred_element_type=F32)


def rotary_table(n_pos):
    half = HEAD // 4
    inv_freq = np.power(ROPE_BASE, -np.arange(half) * 2.0 / (2 * half)).astype(np.float32)
    angles = (np.arange(n_pos, dtype=np.float32)[:, None] * inv_freq[None, :]).astype(np.float64)
    cosine, sine = np.cos(angles), np.sin(angles)
    return np.concatenate([cosine, cosine, sine, sine], axis=1).astype(np.float32)


def fold(vals, op, reduce, share):
    n_cols = vals.shape[1]
    if n_cols % HEAD:
        return jnp.broadcast_to(reduce(vals, axis=-1, keepdims=True) * share, (vals.shape[0], HEAD))
    out = vals[:, 0:HEAD]
    for k in range(1, n_cols // HEAD):
        out = op(out, vals[:, k * HEAD : (k + 1) * HEAD])
    return out


def fused_kernel(
    n_tp,
    n_cp,
    hid,
    wk_a,
    wv_a,
    wq_a,
    wo_a,
    wk,
    wv,
    wq,
    wg,
    wo_l,
    table,
    gain_a,
    gain_l,
    ginner,
    alphas,
    slopes,
    out,
    h1,
    kv_all,
    part,
    summed,
    normed,
    w_buf,
    wo_buf,
    y_buf,
    kvq,
    gate,
    o_buf,
    state,
    state_in,
    res,
    wide,
    gains,
    acc,
    sq_acc,
    row_inv,
    sq_send,
    sq_recv,
    kv_own,
    kv_buf,
    rope,
    sums,
    reduce_send,
    reduce_recv,
    back_send,
    back_recv,
    res_sem,
    out_sem,
    w_sem,
    wo_sem,
    hid_sem,
    rope_sem,
    kv_send,
    kv_recv,
    kv_load,
    state_send,
    state_recv,
    sq_send_sem,
    sq_recv_sem,
    credit,
):
    _, n_tok, model = part.shape
    width = y_buf.shape[1]
    n_heads = width // HEAD
    n_batch = hid.shape[0] // n_tok
    kv_width = wk_a.shape[1]
    group = width // kv_width
    half = n_tok // 2
    rows = res.shape[2]
    per_batch = half // rows
    per_group = per_batch // 4
    layer_pieces = n_batch * per_batch
    pieces = 2 * layer_pieces
    w_cols = w_buf.shape[2]
    wo_cols = wo_buf.shape[2]
    n_wo = model // wo_cols
    kv_tiles = kv_width // w_cols
    a_tiles = 2 * kv_tiles + 8
    last = n_tp - 1
    trip = 2 * last * LEAD
    z = lax.axis_index("tp")
    c = lax.axis_index("cp")

    def hidden_slot(batch):
        return jnp.where(batch == 0, 0, 1)

    def hidden_copy(batch):
        at = hidden_slot(batch)
        return pltpu.make_async_copy(hid.at[pl.ds(pl.multiple_of(batch * n_tok, n_tok), n_tok), :], normed.at[at], hid_sem.at[at])

    def a_tile(unit):
        phase = lax.div(unit, UNITS) - 1
        r = lax.rem(unit, UNITS)
        late = r >= 20
        j = jnp.where(late, r - 20, r)
        is_a = (phase <= 1) & (j < a_tiles) & (jnp.logical_not(late) | (phase == 1))
        batch = jnp.where(late, 3, phase + 1)
        return is_a, batch, j

    def w_cut(weight, tile, slot):
        cols = pl.ds(pl.multiple_of(tile * w_cols, w_cols), w_cols)
        return pltpu.make_async_copy(weight.at[:, cols], w_buf.at[slot], w_sem.at[slot])

    def fetch(unit):
        slot = lax.rem(unit, W_SLOTS)
        r = lax.rem(unit, UNITS)
        phase = lax.div(unit, UNITS) - 1

        @pl.when(phase <= 1)
        def _():
            is_a, _, j = a_tile(unit)

            @pl.when(is_a & (j >= 2 * kv_tiles))
            def _():
                w_cut(wq_a, j - 2 * kv_tiles, slot).start()

            @pl.when(is_a & (j < 2 * kv_tiles))
            def _():
                @pl.when(j < kv_tiles)
                def _():
                    w_cut(wk_a, j, slot).start()

                @pl.when(j >= kv_tiles)
                def _():
                    w_cut(wv_a, j - kv_tiles, slot).start()

        @pl.when(has_projection(phase))
        def _():
            for k, weight in enumerate((wk, wv, wq, wg)):

                @pl.when(lax.div(r, 8) == k)
                def _():
                    w_cut(weight, lax.rem(r, 8), slot).start()

    def has_projection(phase):
        return (phase >= 2) & (phase < 2 + n_batch)

    for i in range(2):
        hidden_copy(i).start()
    for i in range(W_SLOTS):
        fetch(jnp.int32(i))
    table_copy = pltpu.make_async_copy(table.at[pl.ds(pl.multiple_of(c * n_tok, n_tok), n_tok), :], rope.at[0], rope_sem)
    table_copy.start()

    barrier = pltpu.get_barrier_semaphore()
    for k in range(1, n_tp):
        pl.semaphore_signal(barrier, inc=1, device_id={"tp": lax.rem(z + k, n_tp)}, device_id_type=MESH)
    for k in range(1, n_cp):
        pl.semaphore_signal(barrier, inc=1, device_id={"cp": lax.rem(c + k, n_cp)}, device_id_type=MESH)

    gains[0] = gain_a[...]
    gains[1] = gain_l[...]
    table_copy.wait()
    lane = lax.broadcasted_iota(jnp.int32, (n_tok, HEAD), 1)
    cosines = rope[0]
    sines = pltpu.roll(cosines, HEAD // 2, 1)
    rope[0] = jnp.where(lane < HEAD // 2, cosines, 1.0)
    rope[1] = jnp.where(lane < HEAD // 4, -sines, 0.0)
    rope[2] = jnp.where((lane >= HEAD // 4) & (lane < HEAD // 2), sines, 0.0)
    pl.semaphore_wait(barrier, n_tp + n_cp - 2)

    def row_of(g, f):
        return pl.multiple_of(f * half + lax.rem(g, per_batch) * rows, rows)

    def view(ref, g, f):
        return ref.at[lax.rem(lax.div(g, per_batch), 2), pl.ds(row_of(g, f), rows), :]

    def place(f):
        return (z, z + 1, z - 1) if f == 0 else (last - z, z - 1, z + 1)

    def forward(g, f):
        slot = lax.rem(g, RING)
        return pltpu.make_async_remote_copy(
            src_ref=view(part, g, f),
            dst_ref=view(summed, g, f),
            send_sem=reduce_send.at[f, slot],
            recv_sem=reduce_recv.at[f, slot],
            device_id={"tp": place(f)[1]},
            device_id_type=MESH,
        )

    def backward(g, f):
        slot = lax.rem(g, RING)
        return pltpu.make_async_remote_copy(
            src_ref=view(summed, g, f),
            dst_ref=view(summed, g, f),
            send_sem=back_send.at[f, slot],
            recv_sem=back_recv.at[f, slot],
            device_id={"tp": place(f)[2]},
            device_id_type=MESH,
        )

    def hbm_rows(ref, g, f):
        batch = lax.rem(lax.div(g, per_batch), n_batch)
        return ref.at[pl.ds(pl.multiple_of(batch * n_tok + row_of(g, f), rows), rows), :]

    def res_copy(g, f, ref):
        slot = lax.rem(g, 4)
        return pltpu.make_async_copy(hbm_rows(ref, g, f), res.at[f, slot], res_sem.at[f, slot])

    def out_copy(g, f, ref):
        return pltpu.make_async_copy(view(normed, g, f), hbm_rows(ref, g, f), out_sem.at[f, lax.rem(g, 4)])

    def norm_rows(g):
        layer = (g >= layer_pieces).astype(jnp.int32)
        slot = lax.rem(g, 4)
        at = lax.rem(lax.div(g, per_batch), 2)
        alpha = alphas[layer]
        chunks = [slice(i * wo_cols, (i + 1) * wo_cols) for i in range(n_wo)]
        for f in range(2):
            span = pl.ds(row_of(g, f), rows)
            sq = jnp.zeros((rows, wo_cols), F32)
            for cols in chunks:
                vals = alpha * res[f, slot, :, cols].astype(F32) + summed[at, span, cols].astype(F32)
                wide[f, :, cols] = vals
                sq = sq + vals * vals
            scale = lax.rsqrt(jnp.sum(sq, axis=-1, keepdims=True) / model + NORM_EPS)
            for cols in chunks:
                normed[at, span, cols] = (wide[f, :, cols] * scale * gains[layer, :, cols]).astype(BF16)

    def known(g):
        return (g >= 0) & (g < pieces)

    def service(step):
        ahead = step + 3 - trip
        for f in range(2):

            @pl.when((ahead >= 0) & (ahead < layer_pieces))
            def _():
                res_copy(ahead, f, hid).start()

            @pl.when((ahead >= layer_pieces) & (ahead < pieces))
            def _():
                res_copy(ahead, f, h1).start()

        for f in range(2):
            pos = place(f)[0]
            g = step - LEAD * pos

            @pl.when(known(g) & (pos > 0))
            def _():
                forward(g, f).wait_recv()

            @pl.when(known(g) & (pos > 0) & (pos < last))
            def _():
                at = lax.rem(lax.div(g, per_batch), 2)
                span = pl.ds(row_of(g, f), rows)
                part[at, span, :] = part[at, span, :] + summed[at, span, :]

            @pl.when(known(g) & (pos == last))
            def _():
                at = lax.rem(lax.div(g, per_batch), 2)
                span = pl.ds(row_of(g, f), rows)
                summed[at, span, :] = part[at, span, :] + summed[at, span, :]

        for f in range(2):
            pos = place(f)[0]
            g = step - LEAD * pos

            @pl.when(known(g) & (pos < last))
            def _():
                forward(g, f).start()

            @pl.when(known(g) & (pos == last))
            def _():
                backward(g, f).start()

        for f in range(2):
            pos = place(f)[0]
            g = step - LEAD * (2 * last - pos)

            @pl.when(known(g) & (pos < last))
            def _():
                backward(g, f).wait_recv()

            @pl.when(known(g) & (pos < last) & (pos > 0))
            def _():
                backward(g, f).start()

        for f in range(2):
            pos = place(f)[0]
            sent = step - (LEAD * (last - 1) + 3)

            @pl.when(known(sent) & (pos < last))
            def _():
                forward(sent, f).wait_send()

        done = step - trip

        @pl.when(known(done))
        def _():
            for f in range(2):
                pos = place(f)[0]

                @pl.when(pos > 0)
                def _():
                    backward(done, f).wait_send()

                res_copy(done, f, hid).wait()

                @pl.when(done >= 4)
                def _():
                    out_copy(done - 4, f, out).wait()

            norm_rows(done)

            @pl.when(done < layer_pieces)
            def _():
                for f in range(2):
                    out_copy(done, f, h1).start()

            @pl.when(done >= layer_pieces)
            def _():
                for f in range(2):
                    out_copy(done, f, out).start()

    def wo_copy(weight, tile):
        cols = pl.ds(pl.multiple_of(tile * wo_cols, wo_cols), wo_cols)
        slot = lax.rem(tile, 2)
        return pltpu.make_async_copy(weight.at[:, cols], wo_buf.at[slot], wo_sem.at[slot])

    halves = (slice(0, half), slice(half, n_tok))

    def project_a(unit, batch, j):
        slot = lax.rem(unit, W_SLOTS)
        at = hidden_slot(batch)
        w_cut(wk, 0, slot).wait()
        for span in halves:
            acc[span, :] = dot(normed[at, span, :], w_buf[slot])
        store_a(batch, j)

    def project_b(unit, at, which, tile):
        slot = lax.rem(unit, W_SLOTS)
        w_cut(wk, 0, slot).wait()
        cols = pl.ds(pl.multiple_of(tile * w_cols, w_cols), w_cols)

        @pl.when(which < 3)
        def _():
            for span in halves:
                vals = dot(normed[at, span, :], w_buf[slot])
                kvq[which, span, cols] = (vals * jax.nn.sigmoid(vals)).astype(BF16)

        @pl.when(which == 3)
        def _():
            for span in halves:
                gate[span, cols] = jax.nn.sigmoid(dot(normed[at, span, :], w_buf[slot]))

    def query_slot(batch):
        return jnp.where(batch == 3, 2, lax.rem(batch, 2))

    def store_a(batch, j):
        @pl.when((j >= kv_tiles) & (j < 2 * kv_tiles))
        def _():
            cols = pl.ds(pl.multiple_of(j * w_cols, w_cols), w_cols)
            kv_own[:, cols] = acc[...].astype(BF16)

        @pl.when((j < kv_tiles) | (j >= 2 * kv_tiles))
        def _():
            for e in range(w_cols // HEAD):
                raw = acc[:, e * HEAD : (e + 1) * HEAD]
                turned = raw * rope[0] + pltpu.roll(raw, HEAD - HEAD // 4, 1) * rope[1]
                turned = (turned + pltpu.roll(raw, HEAD // 4, 1) * rope[2]).astype(BF16)

                @pl.when(j < kv_tiles)
                def _():
                    kv_own[:, pl.ds(pl.multiple_of(j * w_cols + e * HEAD, HEAD), HEAD)] = turned

                @pl.when(j >= 2 * kv_tiles)
                def _():
                    cols = pl.ds(pl.multiple_of((j - 2 * kv_tiles) * w_cols + e * HEAD, HEAD), HEAD)
                    kvq[query_slot(batch), :, cols] = turned

        @pl.when(j == 2 * kv_tiles - 1)
        def _():
            kv_store(batch).start()
            for mine, theirs in kv_routes:

                @pl.when(c == mine)
                def _():
                    kv_copy(batch, theirs).start()

    def kv_store(batch):
        return pltpu.make_async_copy(kv_own, kv_all.at[batch, c], kv_load.at[n_cp])

    kv_routes = ((0, 1), (0, 2), (1, 3), (2, 3))
    kv_relays = ((2, 0, 3), (3, 1, 2))

    def kv_copy(batch, to):
        return pltpu.make_async_remote_copy(
            src_ref=kv_own,
            dst_ref=kv_all.at[batch, c],
            send_sem=kv_send.at[to],
            recv_sem=kv_recv.at[batch, c],
            device_id={"cp": to},
            device_id_type=MESH,
        )

    def kv_relay(batch, source, to):
        return pltpu.make_async_remote_copy(
            src_ref=kv_all.at[batch, source],
            dst_ref=kv_all.at[batch, source],
            send_sem=kv_send.at[to],
            recv_sem=kv_recv.at[batch, source],
            device_id={"cp": to},
            device_id_type=MESH,
        )

    def kv_fetch(batch, source):
        return pltpu.make_async_copy(kv_all.at[batch, source], kv_buf.at[source], kv_load.at[source])

    def load_kv(batch):
        kv_store(batch).wait()
        for mine, theirs in kv_routes:

            @pl.when(c == mine)
            def _():
                kv_copy(batch, theirs).wait_send()

        for mine, source, theirs in kv_relays:

            @pl.when(c == mine)
            def _():
                kv_relay(batch, source, theirs).wait_recv()
                kv_relay(batch, source, theirs).start()

        for source in range(n_cp):

            @pl.when((source < c) & ((c < 2) | (source != c - 2)))
            def _():
                kv_relay(batch, source, source).wait_recv()

            @pl.when(source <= c)
            def _():
                kv_fetch(batch, source).start()

        for source in range(n_cp):

            @pl.when(source <= c)
            def _():
                kv_fetch(batch, source).wait()

        for mine, source, theirs in kv_relays:

            @pl.when(c == mine)
            def _():
                kv_relay(batch, source, theirs).wait_send()

    def attend(batch, pair):
        kv_head = lax.div(2 * pair, group)
        key_cols = pl.ds(pl.multiple_of(kv_head * HEAD, HEAD), HEAD)
        value_cols = pl.ds(pl.multiple_of(kv_width + kv_head * HEAD, HEAD), HEAD)
        head_cols = [pl.ds(pl.multiple_of((2 * pair + e) * HEAD, HEAD), HEAD) for e in range(2)]
        at = query_slot(batch)
        score_refs = (o_buf, gate)
        top_refs = (sq_acc, row_inv)
        power = math.log2(math.e) / math.sqrt(HEAD)

        def span(j):
            return pl.ds(pl.multiple_of(j * n_tok, n_tok), n_tok)

        rows_at = lax.broadcasted_iota(jnp.int32, (n_tok, n_tok), 0)
        keys_at = lax.broadcasted_iota(jnp.int32, (n_tok, n_tok), 1)
        for e in range(2):
            scores = dot_t(kvq[at, :, head_cols[e]], kv_buf[c, :, key_cols])
            scores = jnp.where(rows_at >= keys_at, scores, -jnp.inf)
            score_refs[e][:, span(c)] = scores
            top_refs[e][...] = fold(scores, jnp.maximum, jnp.max, 1.0)

        def score(j, carry):
            for e in range(2):
                scores = dot_t(kvq[at, :, head_cols[e]], kv_buf[j, :, key_cols])
                score_refs[e][:, span(j)] = scores
                top_refs[e][...] = jnp.maximum(top_refs[e][...], fold(scores, jnp.maximum, jnp.max, 1.0))
            return carry

        lax.fori_loop(0, c, score, 0)
        for e in range(2):
            top_refs[e][...] = jnp.broadcast_to(jnp.max(top_refs[e][...], axis=-1, keepdims=True), (n_tok, HEAD))
            sums[e] = jnp.zeros((n_tok, HEAD), F32)
            acc[:, e * HEAD : (e + 1) * HEAD] = jnp.zeros((n_tok, HEAD), F32)

        lanes = HEAD if n_tok % HEAD == 0 else n_tok

        def weigh(j, carry):
            for e in range(2):
                top = top_refs[e][:, 0:lanes]
                cuts = [pl.ds(pl.multiple_of(j * n_tok + k, lanes), lanes) for k in range(0, n_tok, lanes)]
                parts = [jnp.exp2((score_refs[e][:, cut] - top) * power) for cut in cuts]
                probs = jnp.concatenate(parts, axis=1) if len(parts) > 1 else parts[0]
                sums[e] += fold(probs, jnp.add, jnp.sum, 1.0 / HEAD)
                acc[:, e * HEAD : (e + 1) * HEAD] += dot(probs.astype(BF16), kv_buf[j, :, value_cols])
            return carry

        lax.fori_loop(0, c + 1, weigh, 0)
        for e in range(2):
            total = jnp.sum(sums[e], axis=-1, keepdims=True)
            y_buf[:, head_cols[e]] = (acc[:, e * HEAD : (e + 1) * HEAD] / total).astype(BF16)

    def out_project(phase, tile):
        wo_copy(wo_a, tile).wait()
        slot = lax.rem(tile, 2)
        cols = pl.ds(pl.multiple_of(tile * wo_cols, wo_cols), wo_cols)
        at = lax.rem(phase + 1, 2)
        part[at, :, cols] = dot(y_buf[...], wo_buf[slot]).astype(BF16)

    def state_copy():
        return pltpu.make_async_remote_copy(
            src_ref=state,
            dst_ref=state_in,
            send_sem=state_send,
            recv_sem=state_recv,
            device_id={"cp": c + 1},
            device_id_type=MESH,
        )

    def local_lightning(pair):
        def one_head(h):
            cols = pl.ds(pl.multiple_of(h * HEAD, HEAD), HEAD)
            rate = slopes[h]
            key, value, query = kvq[0, :, cols], kvq[1, :, cols], kvq[2, :, cols]
            part_rows = n_tok // 3
            for i in range(3):
                span = slice(i * part_rows, (i + 1) * part_rows)
                upto = slice(0, (i + 1) * part_rows)
                scores = dot_t(query[span], key[upto])
                gap = lax.broadcasted_iota(jnp.int32, scores.shape, 0) - lax.broadcasted_iota(jnp.int32, scores.shape, 1) + i * part_rows
                decay = jnp.where(gap >= 0, jnp.exp(-rate * gap.astype(F32)), 0.0)
                o_buf[span, cols] = dot((scores * decay).astype(BF16), value[upto])
            to_end = (n_tok - 1 - lax.broadcasted_iota(jnp.int32, (n_tok, HEAD), 0)).astype(F32)
            faded = key.astype(F32) * jnp.exp(-rate * to_end)
            state[h] = dot(faded.T.astype(BF16), value)

        one_head(2 * pair)
        one_head(2 * pair + 1)

    def add_incoming():
        def head(h, carry):
            state[h] = state_in[h] * jnp.exp(jnp.zeros((HEAD, HEAD), F32) - slopes[h] * n_tok) + state[h]
            return carry

        lax.fori_loop(0, n_heads, head, 0)

    def send_state(batch):
        @pl.when(batch > 0)
        def _():
            pl.semaphore_wait(credit, 1)

        state_copy().start()

    def sq_copy(batch, k):
        peer = lax.rem(z + k, n_tp)
        return pltpu.make_async_remote_copy(
            src_ref=sq_send,
            dst_ref=sq_recv.at[batch, z],
            send_sem=sq_send_sem.at[k],
            recv_sem=sq_recv_sem.at[batch, z],
            device_id={"tp": peer},
            device_id_type=MESH,
        )

    def sq_arrival(batch, k):
        source = lax.rem(z + n_tp - k, n_tp)
        return pltpu.make_async_remote_copy(
            src_ref=sq_send,
            dst_ref=sq_recv.at[batch, source],
            send_sem=sq_send_sem.at[k],
            recv_sem=sq_recv_sem.at[batch, source],
            device_id={"tp": source},
            device_id_type=MESH,
        )

    def add_earlier(batch):
        @pl.when(c == n_cp - 1)
        def _():
            state_copy().wait_recv()

        @pl.when(c < n_cp - 1)
        def _():
            state_copy().wait_send()

        sq_acc[...] = jnp.zeros_like(sq_acc)

        def cols_of(h):
            return pl.ds(pl.multiple_of(h * HEAD, HEAD), HEAD)

        def head_pair(i, carry):
            for h in (2 * i, 2 * i + 1):
                steps = (lax.broadcasted_iota(jnp.int32, (n_tok, HEAD), 0) + 1).astype(F32)
                prior = dot(kvq[2, :, cols_of(h)], state_in[h].astype(BF16))
                vals = o_buf[:, cols_of(h)] + prior * jnp.exp(-slopes[h] * steps)
                o_buf[:, cols_of(h)] = vals
                sq_acc[...] += vals * vals
            return carry

        def head(h, carry):
            vals = o_buf[:, cols_of(h)]
            sq_acc[...] += vals * vals
            return carry

        @pl.when(c > 0)
        def _():
            lax.fori_loop(0, n_heads // 2, head_pair, 0)

        @pl.when(c == 0)
        def _():
            lax.fori_loop(0, n_heads, head, 0)

        @pl.when((c > 0) & (batch < n_batch - 1))
        def _():
            pl.semaphore_signal(credit, inc=1, device_id={"cp": c - 1}, device_id_type=MESH)

        row_sq = jnp.broadcast_to(jnp.sum(sq_acc[...], axis=-1, keepdims=True), (n_tok, HEAD))
        sq_send[...] = row_sq.T[0:8, :]
        sq_recv[batch, z] = sq_send[...]
        for k in range(1, n_tp):
            sq_copy(batch, k).start()

    def finish_lightning(batch):
        for k in range(1, n_tp):
            sq_arrival(batch, k).wait_recv()
        for k in range(1, n_tp):
            sq_copy(batch, k).wait_send()
        total = sq_recv[batch, 0]
        for k in range(1, n_tp):
            total = total + sq_recv[batch, k]
        tall = jnp.broadcast_to(total[0:1, :], (HEAD, n_tok)).T
        row_inv[...] = lax.rsqrt(tall / (width * n_tp) + NORM_EPS)

        def head(h, carry):
            cols = pl.ds(pl.multiple_of(h * HEAD, HEAD), HEAD)
            y_buf[:, cols] = (o_buf[:, cols] * row_inv[...] * ginner[h] * gate[:, cols]).astype(BF16)
            return carry

        lax.fori_loop(0, n_heads, head, 0)

    def unit_body(unit, carry):
        phase = lax.div(unit, UNITS) - 1
        r = lax.rem(unit, UNITS)
        which = lax.div(r, 8)
        tile = lax.rem(r, 8)
        first_layer = phase < n_batch - 1
        second_layer = (phase >= 3) & (phase < 3 + n_batch)
        projects = has_projection(phase)

        @pl.when(lax.rem(tile, 3) == 0)
        def _():
            part_of = lax.div(tile, 3)

            def one(i, inner):
                service(phase * per_batch + which * per_group + part_of * (per_group // 3) + i)
                return inner

            if per_group == 3:
                one(0, 0)
            else:
                lax.fori_loop(0, per_group // 3, one, 0)

        @pl.when(lax.rem(r, 4) == 0)
        def _():
            @pl.when(phase <= 2)
            def _():
                for at_phase, at_r, batch in ((0, 0, 1), (1, 0, 2), (1, 20, 3)):

                    @pl.when((phase == at_phase) & (r == at_r))
                    def _():
                        hidden_copy(batch).wait()

                for at_phase, batch in ((0, 2), (1, 3)):

                    @pl.when((phase == at_phase) & (r == 12))
                    def _():
                        hidden_copy(batch).start()

                @pl.when(r == 8)
                def _():
                    for i in range(2):
                        wo_copy(wo_a, i).start()

            @pl.when(second_layer)
            def _():
                @pl.when((r == 4) & (c == 1) | (r == 8) & (c == 2))
                def _():
                    state_copy().wait_recv()
                    add_incoming()
                    send_state(phase - 3)

                @pl.when(r == 8)
                def _():
                    for i in range(2):
                        wo_copy(wo_l, i).start()

                @pl.when(r == 12)
                def _():
                    add_earlier(phase - 3)

                @pl.when(r == 16)
                def _():
                    finish_lightning(phase - 3)

        @pl.when(first_layer & (r < 20))
        def _():
            @pl.when(r == jnp.where(phase < 0, 12, jnp.where(phase <= 1, 10, 0)))
            def _():
                load_kv(phase + 1)

            k = r - 10
            by_five = lax.rem(r, 5)
            pair = jnp.where(phase < 0, 2 * (r - 12), jnp.where(phase <= 1, k - lax.div(k, 5), 2 * lax.div(r, 5) + (by_five == 2)))
            single = (phase >= 0) & (phase <= 1) & (r >= 10) & (by_five != 4) | (phase == 2) & ((by_five == 0) | (by_five == 2))
            n_here = jnp.where((phase < 0) & (r >= 12) & (r < 16), 2, jnp.where(single, 1, 0))

            def one_pair(i, inner):
                attend(phase + 1, pair + i)
                return inner

            lax.fori_loop(0, n_here, one_pair, 0)

        wo_tile = r - jnp.where(first_layer, 20, 16)

        @pl.when((wo_tile >= 0) & (wo_tile < n_wo) & (phase < 3 + n_batch))
        def _():
            out_project(phase, wo_tile)

            @pl.when((wo_tile < n_wo - 2) & first_layer)
            def _():
                wo_copy(wo_a, wo_tile + 2).start()

            @pl.when((wo_tile < n_wo - 2) & second_layer)
            def _():
                wo_copy(wo_l, wo_tile + 2).start()

        @pl.when(phase <= 1)
        def _():
            is_a, a_batch, a_j = a_tile(unit)

            @pl.when(is_a)
            def _():
                project_a(unit, a_batch, a_j)

        @pl.when(projects)
        def _():
            project_b(unit, lax.rem(phase, 2), which, tile)

            @pl.when(which == 3)
            def _():
                local_lightning(tile)

                @pl.when((tile == 7) & (c == 0))
                def _():
                    send_state(phase - 2)

        fetch(unit + W_SLOTS)
        return carry

    hidden_copy(0).wait()
    n_phases = 2 * n_batch + 2
    lax.fori_loop(0, n_phases * UNITS, unit_body, 0)
    for f in range(2):
        for k in range(4):
            out_copy(pieces - 4 + k, f, out).wait()


def copy_kernel(blocks, src, dst, buf, read_sem, write_sem):
    rows = src.shape[0] // blocks

    def read(i):
        span = pl.ds(i * rows, rows)
        return pltpu.make_async_copy(src.at[span, :], buf.at[span, :], read_sem.at[i])

    def write(i):
        span = pl.ds(i * rows, rows)
        return pltpu.make_async_copy(buf.at[span, :], dst.at[span, :], write_sem.at[i])

    for i in range(blocks):
        read(i).start()
    for i in range(blocks):
        read(i).wait()
        write(i).start()
    for i in range(blocks):
        write(i).wait()


def plain_copy(array, blocks):
    shape = jax.ShapeDtypeStruct(array.shape, array.dtype)
    return pl.pallas_call(
        functools.partial(copy_kernel, blocks),
        out_shape=shape,
        in_specs=[ANY],
        out_specs=ANY,
        scratch_shapes=[pltpu.VMEM(array.shape, array.dtype), pltpu.SemaphoreType.DMA((blocks,)), pltpu.SemaphoreType.DMA((blocks,))],
        compiler_params=pltpu.CompilerParams(vmem_limit_bytes=48 * 1024 * 1024),
    )(array)


def fused_layers(hid, weights, gains, ginner, alphas, slopes, n_tok, n_tp, n_cp):
    n_rows, model = hid.shape
    width = weights[2].shape[1]
    kv_width = weights[0].shape[1]
    n_batch = n_rows // n_tok
    n_heads = width // HEAD
    rows = n_tok // 24
    w_cols = width // 8
    wo_cols = model // 12
    vmem, dma = pltpu.VMEM, pltpu.SemaphoreType.DMA
    scratch = [
        vmem((2, n_tok, model), BF16),
        vmem((2, n_tok, model), BF16),
        vmem((2, n_tok, model), BF16),
        vmem((W_SLOTS, model, w_cols), BF16),
        vmem((2, width, wo_cols), BF16),
        vmem((n_tok, width), BF16),
        vmem((3, n_tok, width), BF16),
        vmem((n_tok, width), F32),
        vmem((n_tok, width), F32),
        vmem((n_heads, HEAD, HEAD), F32),
        vmem((n_heads, HEAD, HEAD), F32),
        vmem((2, 4, rows, model), BF16),
        vmem((2, rows, model), F32),
        vmem((2, 1, model), F32),
        vmem((n_tok, w_cols), F32),
        vmem((n_tok, HEAD), F32),
        vmem((n_tok, HEAD), F32),
        vmem((8, n_tok), F32),
        vmem((n_batch, n_tp, 8, n_tok), F32),
        vmem((n_tok, 2 * kv_width), BF16),
        vmem((n_cp, n_tok, 2 * kv_width), BF16),
        vmem((3, n_tok, HEAD), F32),
        vmem((2, n_tok, HEAD), F32),
        dma((2, RING)),
        dma((2, RING)),
        dma((2, RING)),
        dma((2, RING)),
        dma((2, 4)),
        dma((2, 4)),
        dma((W_SLOTS,)),
        dma((2,)),
        dma((2,)),
        dma,
        dma((n_cp,)),
        dma((n_batch, n_cp)),
        dma((n_cp + 1,)),
        dma,
        dma,
        dma((n_tp,)),
        dma((n_batch, n_tp)),
        pltpu.SemaphoreType.REGULAR,
    ]
    flops = 2 * n_rows * model * width * 8
    return pl.pallas_call(
        functools.partial(fused_kernel, n_tp, n_cp),
        out_shape=[
            jax.ShapeDtypeStruct((n_rows, model), BF16),
            jax.ShapeDtypeStruct((n_rows, model), BF16),
            jax.ShapeDtypeStruct((n_batch, n_cp, n_tok, 2 * kv_width), BF16),
        ],
        in_specs=[ANY] * 11 + [VMEM] * 3 + [SMEM] * 2,
        out_specs=[ANY] * 3,
        scratch_shapes=scratch,
        compiler_params=pltpu.CompilerParams(collective_id=0, has_side_effects=True, vmem_limit_bytes=67043328),
        cost_estimate=pl.CostEstimate(flops=flops, bytes_accessed=12 * n_rows * model, transcendentals=0),
    )(hid, *weights, rotary_table(n_tok * n_cp), *gains, ginner, alphas, slopes)


def solution(mesh):
    n_tp, n_cp = mesh.shape["tp"], mesh.shape["cp"]

    def body(hidden, alphas, wq_attn, wk_attn, wv_attn, wo_attn, gain_attn, wq_lin, wk_lin, wv_lin, wg_lin, slopes, gain_inner, wo_lin, gain_lin):
        n_batch, n_tok, model = hidden.shape
        flat = hidden.reshape(n_batch * n_tok, model)
        gains = (gain_attn[None, :], gain_lin[None, :])
        weights = (wk_attn, wv_attn, wq_attn, wo_attn, wk_lin, wv_lin, wq_lin, wg_lin, wo_lin)
        outs = fused_layers(flat, weights, gains, gain_inner.reshape(-1, 1, HEAD), alphas, slopes, n_tok, n_tp, n_cp)
        return plain_copy(outs[0], 16).reshape(hidden.shape)

    act_spec = P("dp", "cp", None)
    rep_spec = P()
    col_spec = P(None, "tp")
    row_spec = P("tp", None)
    vec_spec = P("tp")
    in_specs = (act_spec, rep_spec, col_spec, col_spec, col_spec, row_spec, rep_spec, col_spec, col_spec, col_spec, col_spec, vec_spec, vec_spec, row_spec, rep_spec)
    return jax.shard_map(body, mesh=mesh, in_specs=in_specs, out_specs=act_spec, check_vma=False)
```

```python
import functools
import math

import jax
import jax.numpy as jnp
import numpy as np
from jax import lax
from jax.experimental import pallas as pl
from jax.experimental.pallas import tpu as pltpu
from jax.sharding import PartitionSpec as P

ROPE_BASE = 10000000.0
NORM_EPS = 1e-5
HEAD = 128
MESH = pl.DeviceIdType.MESH
F32 = jnp.float32
BF16 = jnp.bfloat16
ANY = pl.BlockSpec(memory_space=pl.ANY)
VMEM = pl.BlockSpec(memory_space=pltpu.VMEM)
SMEM = pl.BlockSpec(memory_space=pltpu.SMEM)

LEAD = 2
RING = 16
UNITS = 32
W_SLOTS = 3


def dot(lhs, rhs):
    return jnp.dot(lhs, rhs, preferred_element_type=F32)


def dot_t(lhs, rhs):
    return lax.dot_general(lhs, rhs, (((1,), (1,)), ((), ())), preferred_element_type=F32)


def rotary_table(n_pos):
    half = HEAD // 4
    inv_freq = np.power(ROPE_BASE, -np.arange(half) * 2.0 / (2 * half)).astype(np.float32)
    angles = (np.arange(n_pos, dtype=np.float32)[:, None] * inv_freq[None, :]).astype(np.float64)
    cosine, sine = np.cos(angles), np.sin(angles)
    return np.concatenate([cosine, cosine, sine, sine], axis=1).astype(np.float32)


def fold(vals, op, reduce, share):
    n_cols = vals.shape[1]
    if n_cols % HEAD:
        return jnp.broadcast_to(reduce(vals, axis=-1, keepdims=True) * share, (vals.shape[0], HEAD))
    out = vals[:, 0:HEAD]
    for k in range(1, n_cols // HEAD):
        out = op(out, vals[:, k * HEAD : (k + 1) * HEAD])
    return out


def fused_kernel(
    n_tp,
    n_cp,
    hid,
    wk_a,
    wv_a,
    wq_a,
    wo_a,
    wk,
    wv,
    wq,
    wg,
    wo_l,
    table,
    gain_a,
    gain_l,
    ginner,
    alphas,
    slopes,
    out,
    h1,
    kv_all,
    part,
    summed,
    normed,
    w_buf,
    wo_buf,
    y_buf,
    kvq,
    gate,
    o_buf,
    state,
    state_in,
    res,
    wide,
    gains,
    acc,
    sq_acc,
    row_inv,
    sq_send,
    sq_recv,
    kv_own,
    kv_buf,
    rope,
    sums,
    reduce_send,
    reduce_recv,
    back_send,
    back_recv,
    res_sem,
    out_sem,
    w_sem,
    wo_sem,
    hid_sem,
    rope_sem,
    kv_send,
    kv_recv,
    kv_load,
    state_send,
    state_recv,
    sq_send_sem,
    sq_recv_sem,
    credit,
):
    _, n_tok, model = part.shape
    width = y_buf.shape[1]
    n_heads = width // HEAD
    n_batch = hid.shape[0] // n_tok
    kv_width = wk_a.shape[1]
    group = width // kv_width
    half = n_tok // 2
    rows = res.shape[2]
    per_batch = half // rows
    per_group = per_batch // 4
    layer_pieces = n_batch * per_batch
    pieces = 2 * layer_pieces
    w_cols = w_buf.shape[2]
    wo_cols = wo_buf.shape[2]
    n_wo = model // wo_cols
    kv_tiles = kv_width // w_cols
    a_tiles = 2 * kv_tiles + 8
    last = n_tp - 1
    trip = 2 * last * LEAD
    z = lax.axis_index("tp")
    c = lax.axis_index("cp")

    def hidden_slot(batch):
        return jnp.where(batch == 0, 0, 1)

    def hidden_copy(batch):
        at = hidden_slot(batch)
        return pltpu.make_async_copy(hid.at[pl.ds(pl.multiple_of(batch * n_tok, n_tok), n_tok), :], normed.at[at], hid_sem.at[at])

    def a_tile(unit):
        phase = lax.div(unit, UNITS) - 1
        r = lax.rem(unit, UNITS)
        late = r >= 20
        j = jnp.where(late, r - 20, r)
        is_a = (phase <= 1) & (j < a_tiles) & (jnp.logical_not(late) | (phase == 1))
        batch = jnp.where(late, 3, phase + 1)
        return is_a, batch, j

    def w_cut(weight, tile, slot):
        cols = pl.ds(pl.multiple_of(tile * w_cols, w_cols), w_cols)
        return pltpu.make_async_copy(weight.at[:, cols], w_buf.at[slot], w_sem.at[slot])

    def fetch(unit):
        slot = lax.rem(unit, W_SLOTS)
        r = lax.rem(unit, UNITS)
        phase = lax.div(unit, UNITS) - 1

        @pl.when(phase <= 1)
        def _():
            is_a, _, j = a_tile(unit)

            @pl.when(is_a & (j >= 2 * kv_tiles))
            def _():
                w_cut(wq_a, j - 2 * kv_tiles, slot).start()

            @pl.when(is_a & (j < 2 * kv_tiles))
            def _():
                @pl.when(j < kv_tiles)
                def _():
                    w_cut(wk_a, j, slot).start()

                @pl.when(j >= kv_tiles)
                def _():
                    w_cut(wv_a, j - kv_tiles, slot).start()

        @pl.when(has_projection(phase))
        def _():
            for k, weight in enumerate((wk, wv, wq, wg)):

                @pl.when(lax.div(r, 8) == k)
                def _():
                    w_cut(weight, lax.rem(r, 8), slot).start()

    def has_projection(phase):
        return (phase >= 2) & (phase < 2 + n_batch)

    hidden_copy(0).start()
    fetch(jnp.int32(0))
    table_copy = pltpu.make_async_copy(table.at[pl.ds(pl.multiple_of(c * n_tok, n_tok), n_tok), :], rope.at[0], rope_sem)
    table_copy.start()

    barrier = pltpu.get_barrier_semaphore()
    for k in range(1, n_tp):
        pl.semaphore_signal(barrier, inc=1, device_id={"tp": lax.rem(z + k, n_tp)}, device_id_type=MESH)
    for k in range(1, n_cp):
        pl.semaphore_signal(barrier, inc=1, device_id={"cp": lax.rem(c + k, n_cp)}, device_id_type=MESH)

    gains[0] = gain_a[...]
    gains[1] = gain_l[...]
    table_copy.wait()
    lane = lax.broadcasted_iota(jnp.int32, (n_tok, HEAD), 1)
    cosines = rope[0]
    sines = pltpu.roll(cosines, HEAD // 2, 1)
    rope[0] = jnp.where(lane < HEAD // 2, cosines, 1.0)
    rope[1] = jnp.where(lane < HEAD // 4, -sines, 0.0)
    rope[2] = jnp.where((lane >= HEAD // 4) & (lane < HEAD // 2), sines, 0.0)
    for i in range(1, W_SLOTS):
        fetch(jnp.int32(i))

    def row_of(g, f):
        return pl.multiple_of(f * half + lax.rem(g, per_batch) * rows, rows)

    def view(ref, g, f):
        return ref.at[lax.rem(lax.div(g, per_batch), 2), pl.ds(row_of(g, f), rows), :]

    def place(f):
        return (z, z + 1, z - 1) if f == 0 else (last - z, z - 1, z + 1)

    def forward(g, f):
        slot = lax.rem(g, RING)
        return pltpu.make_async_remote_copy(
            src_ref=view(part, g, f),
            dst_ref=view(summed, g, f),
            send_sem=reduce_send.at[f, slot],
            recv_sem=reduce_recv.at[f, slot],
            device_id={"tp": place(f)[1]},
            device_id_type=MESH,
        )

    def backward(g, f):
        slot = lax.rem(g, RING)
        return pltpu.make_async_remote_copy(
            src_ref=view(summed, g, f),
            dst_ref=view(summed, g, f),
            send_sem=back_send.at[f, slot],
            recv_sem=back_recv.at[f, slot],
            device_id={"tp": place(f)[2]},
            device_id_type=MESH,
        )

    def hbm_rows(ref, g, f):
        batch = lax.rem(lax.div(g, per_batch), n_batch)
        return ref.at[pl.ds(pl.multiple_of(batch * n_tok + row_of(g, f), rows), rows), :]

    def res_copy(g, f, ref):
        slot = lax.rem(g, 4)
        return pltpu.make_async_copy(hbm_rows(ref, g, f), res.at[f, slot], res_sem.at[f, slot])

    def out_copy(g, f, ref):
        return pltpu.make_async_copy(view(normed, g, f), hbm_rows(ref, g, f), out_sem.at[f, lax.rem(g, 4)])

    def norm_rows(g):
        layer = (g >= layer_pieces).astype(jnp.int32)
        slot = lax.rem(g, 4)
        at = lax.rem(lax.div(g, per_batch), 2)
        alpha = alphas[layer]
        chunks = [slice(i * wo_cols, (i + 1) * wo_cols) for i in range(n_wo)]
        for f in range(2):
            span = pl.ds(row_of(g, f), rows)
            sq = jnp.zeros((rows, wo_cols), F32)
            for cols in chunks:
                vals = alpha * res[f, slot, :, cols].astype(F32) + summed[at, span, cols].astype(F32)
                wide[f, :, cols] = vals
                sq = sq + vals * vals
            scale = lax.rsqrt(jnp.sum(sq, axis=-1, keepdims=True) / model + NORM_EPS)
            for cols in chunks:
                normed[at, span, cols] = (wide[f, :, cols] * scale * gains[layer, :, cols]).astype(BF16)

    def known(g):
        return (g >= 0) & (g < pieces)

    def service(step):
        ahead = step + 3 - trip
        for f in range(2):

            @pl.when((ahead >= 0) & (ahead < layer_pieces))
            def _():
                res_copy(ahead, f, hid).start()

            @pl.when((ahead >= layer_pieces) & (ahead < pieces))
            def _():
                res_copy(ahead, f, h1).start()

        for f in range(2):
            pos = place(f)[0]
            g = step - LEAD * pos

            @pl.when(known(g) & (pos > 0))
            def _():
                forward(g, f).wait_recv()

            @pl.when(known(g) & (pos > 0) & (pos < last))
            def _():
                at = lax.rem(lax.div(g, per_batch), 2)
                span = pl.ds(row_of(g, f), rows)
                part[at, span, :] = part[at, span, :] + summed[at, span, :]

            @pl.when(known(g) & (pos == last))
            def _():
                at = lax.rem(lax.div(g, per_batch), 2)
                span = pl.ds(row_of(g, f), rows)
                summed[at, span, :] = part[at, span, :] + summed[at, span, :]

        for f in range(2):
            pos = place(f)[0]
            g = step - LEAD * pos

            @pl.when(known(g) & (pos < last))
            def _():
                forward(g, f).start()

            @pl.when(known(g) & (pos == last))
            def _():
                backward(g, f).start()

        for f in range(2):
            pos = place(f)[0]
            g = step - LEAD * (2 * last - pos)

            @pl.when(known(g) & (pos < last))
            def _():
                backward(g, f).wait_recv()

            @pl.when(known(g) & (pos < last) & (pos > 0))
            def _():
                backward(g, f).start()

        for f in range(2):
            pos = place(f)[0]
            sent = step - (LEAD * (last - 1) + 3)

            @pl.when(known(sent) & (pos < last))
            def _():
                forward(sent, f).wait_send()

        done = step - trip

        @pl.when(known(done))
        def _():
            for f in range(2):
                pos = place(f)[0]

                @pl.when(pos > 0)
                def _():
                    backward(done, f).wait_send()

                res_copy(done, f, hid).wait()

                @pl.when(done >= 4)
                def _():
                    out_copy(done - 4, f, out).wait()

            norm_rows(done)

            @pl.when(done < layer_pieces)
            def _():
                for f in range(2):
                    out_copy(done, f, h1).start()

            @pl.when(done >= layer_pieces)
            def _():
                for f in range(2):
                    out_copy(done, f, out).start()

    def wo_copy(weight, tile):
        cols = pl.ds(pl.multiple_of(tile * wo_cols, wo_cols), wo_cols)
        slot = lax.rem(tile, 2)
        return pltpu.make_async_copy(weight.at[:, cols], wo_buf.at[slot], wo_sem.at[slot])

    halves = (slice(0, half), slice(half, n_tok))

    def project_a(unit, batch, j):
        slot = lax.rem(unit, W_SLOTS)
        at = hidden_slot(batch)
        w_cut(wk, 0, slot).wait()
        for span in halves:
            acc[span, :] = dot(normed[at, span, :], w_buf[slot])
        store_a(batch, j)

    def project_b(unit, at, which, tile):
        slot = lax.rem(unit, W_SLOTS)
        w_cut(wk, 0, slot).wait()
        cols = pl.ds(pl.multiple_of(tile * w_cols, w_cols), w_cols)

        @pl.when(which < 3)
        def _():
            for span in halves:
                vals = dot(normed[at, span, :], w_buf[slot])
                kvq[which, span, cols] = (vals * jax.nn.sigmoid(vals)).astype(BF16)

        @pl.when(which == 3)
        def _():
            for span in halves:
                gate[span, cols] = jax.nn.sigmoid(dot(normed[at, span, :], w_buf[slot]))

    def query_slot(batch):
        return jnp.where(batch == 3, 2, lax.rem(batch, 2))

    def store_a(batch, j):
        @pl.when((j >= kv_tiles) & (j < 2 * kv_tiles))
        def _():
            cols = pl.ds(pl.multiple_of(j * w_cols, w_cols), w_cols)
            kv_own[:, cols] = acc[...].astype(BF16)

        @pl.when((j < kv_tiles) | (j >= 2 * kv_tiles))
        def _():
            for e in range(w_cols // HEAD):
                raw = acc[:, e * HEAD : (e + 1) * HEAD]
                turned = raw * rope[0] + pltpu.roll(raw, HEAD - HEAD // 4, 1) * rope[1]
                turned = (turned + pltpu.roll(raw, HEAD // 4, 1) * rope[2]).astype(BF16)

                @pl.when(j < kv_tiles)
                def _():
                    kv_own[:, pl.ds(pl.multiple_of(j * w_cols + e * HEAD, HEAD), HEAD)] = turned

                @pl.when(j >= 2 * kv_tiles)
                def _():
                    cols = pl.ds(pl.multiple_of((j - 2 * kv_tiles) * w_cols + e * HEAD, HEAD), HEAD)
                    kvq[query_slot(batch), :, cols] = turned

        @pl.when(j == 2 * kv_tiles - 1)
        def _():
            kv_store(batch).start()
            for mine, theirs in kv_routes:

                @pl.when(c == mine)
                def _():
                    kv_copy(batch, theirs).start()

    def kv_store(batch):
        return pltpu.make_async_copy(kv_own, kv_all.at[batch, c], kv_load.at[n_cp])

    kv_routes = ((0, 1), (0, 2), (1, 3), (2, 3))
    kv_relays = ((2, 0, 3), (3, 1, 2))

    def kv_copy(batch, to):
        return pltpu.make_async_remote_copy(
            src_ref=kv_own,
            dst_ref=kv_all.at[batch, c],
            send_sem=kv_send.at[to],
            recv_sem=kv_recv.at[batch, c],
            device_id={"cp": to},
            device_id_type=MESH,
        )

    def kv_relay(batch, source, to):
        return pltpu.make_async_remote_copy(
            src_ref=kv_all.at[batch, source],
            dst_ref=kv_all.at[batch, source],
            send_sem=kv_send.at[to],
            recv_sem=kv_recv.at[batch, source],
            device_id={"cp": to},
            device_id_type=MESH,
        )

    def kv_fetch(batch, source):
        return pltpu.make_async_copy(kv_all.at[batch, source], kv_buf.at[source], kv_load.at[source])

    def relay_kv(batch):
        for mine, source, theirs in kv_relays:

            @pl.when(c == mine)
            def _():
                kv_relay(batch, source, theirs).wait_recv()
                kv_relay(batch, source, theirs).start()

    def load_kv(batch):
        kv_store(batch).wait()
        for mine, theirs in kv_routes:

            @pl.when(c == mine)
            def _():
                kv_copy(batch, theirs).wait_send()

        for source in range(n_cp):

            @pl.when((source < c) & ((c < 2) | (source != c - 2)))
            def _():
                kv_relay(batch, source, source).wait_recv()

            @pl.when(source <= c)
            def _():
                kv_fetch(batch, source).start()

        for source in range(n_cp):

            @pl.when(source <= c)
            def _():
                kv_fetch(batch, source).wait()

        for mine, source, theirs in kv_relays:

            @pl.when(c == mine)
            def _():
                kv_relay(batch, source, theirs).wait_send()

    def attend(batch, pair):
        kv_head = lax.div(2 * pair, group)
        key_cols = pl.ds(pl.multiple_of(kv_head * HEAD, HEAD), HEAD)
        value_cols = pl.ds(pl.multiple_of(kv_width + kv_head * HEAD, HEAD), HEAD)
        head_cols = [pl.ds(pl.multiple_of((2 * pair + e) * HEAD, HEAD), HEAD) for e in range(2)]
        at = query_slot(batch)
        score_refs = (o_buf, gate)
        top_refs = (sq_acc, row_inv)
        power = math.log2(math.e) / math.sqrt(HEAD)

        def span(j):
            return pl.ds(pl.multiple_of(j * n_tok, n_tok), n_tok)

        tall = n_tok // 3
        lanes = HEAD if n_tok % HEAD == 0 else tall
        tiles = [(slice(i * tall, (i + 1) * tall), slice(0, (i + 1) * tall), i) for i in range(3)]
        own = [pl.ds(pl.multiple_of(c * n_tok + k, lanes), lanes) for k in range(0, n_tok, lanes)]
        for rows_of, upto, i in tiles:
            for e in range(2):
                scores = dot_t(kvq[at, rows_of, head_cols[e]], kv_buf[c, upto, key_cols])
                rows_at = lax.broadcasted_iota(jnp.int32, scores.shape, 0) + i * tall
                scores = jnp.where(rows_at >= lax.broadcasted_iota(jnp.int32, scores.shape, 1), scores, -jnp.inf)
                for k in range(i + 1):
                    score_refs[e][rows_of, own[k]] = scores[:, k * tall : (k + 1) * tall]
                top_refs[e][rows_of, :] = fold(scores, jnp.maximum, jnp.max, 1.0)

        def score(j, carry):
            for e in range(2):
                scores = dot_t(kvq[at, :, head_cols[e]], kv_buf[j, :, key_cols])
                score_refs[e][:, span(j)] = scores
                top_refs[e][...] = jnp.maximum(top_refs[e][...], fold(scores, jnp.maximum, jnp.max, 1.0))
            return carry

        lax.fori_loop(0, c, score, 0)
        for e in range(2):
            top_refs[e][...] = jnp.broadcast_to(jnp.max(top_refs[e][...], axis=-1, keepdims=True), (n_tok, HEAD))

        for rows_of, upto, i in tiles:
            for e in range(2):
                top = top_refs[e][rows_of, 0:lanes]
                parts = [jnp.exp2((score_refs[e][rows_of, own[k]] - top) * power) for k in range(i + 1)]
                probs = jnp.concatenate(parts, axis=1) if i else parts[0]
                sums[e, rows_of, :] = fold(probs, jnp.add, jnp.sum, 1.0 / HEAD)
                acc[rows_of, e * HEAD : (e + 1) * HEAD] = dot(probs.astype(BF16), kv_buf[c, upto, value_cols])

        def weigh(j, carry):
            for e in range(2):
                top = top_refs[e][:, 0:lanes]
                cuts = [pl.ds(pl.multiple_of(j * n_tok + k, lanes), lanes) for k in range(0, n_tok, lanes)]
                parts = [jnp.exp2((score_refs[e][:, cut] - top) * power) for cut in cuts]
                probs = jnp.concatenate(parts, axis=1) if len(parts) > 1 else parts[0]
                sums[e] += fold(probs, jnp.add, jnp.sum, 1.0 / HEAD)
                acc[:, e * HEAD : (e + 1) * HEAD] += dot(probs.astype(BF16), kv_buf[j, :, value_cols])
            return carry

        lax.fori_loop(0, c, weigh, 0)
        for e in range(2):
            total = jnp.sum(sums[e], axis=-1, keepdims=True)
            y_buf[:, head_cols[e]] = (acc[:, e * HEAD : (e + 1) * HEAD] / total).astype(BF16)

    def out_project(phase, tile):
        wo_copy(wo_a, tile).wait()
        slot = lax.rem(tile, 2)
        cols = pl.ds(pl.multiple_of(tile * wo_cols, wo_cols), wo_cols)
        at = lax.rem(phase + 1, 2)
        part[at, :, cols] = dot(y_buf[...], wo_buf[slot]).astype(BF16)

    def state_copy():
        return pltpu.make_async_remote_copy(
            src_ref=state,
            dst_ref=state_in,
            send_sem=state_send,
            recv_sem=state_recv,
            device_id={"cp": c + 1},
            device_id_type=MESH,
        )

    def local_lightning(pair):
        def one_head(h):
            cols = pl.ds(pl.multiple_of(h * HEAD, HEAD), HEAD)
            rate = slopes[h]
            key, value, query = kvq[0, :, cols], kvq[1, :, cols], kvq[2, :, cols]
            part_rows = n_tok // 3
            for i in range(3):
                span = slice(i * part_rows, (i + 1) * part_rows)
                upto = slice(0, (i + 1) * part_rows)
                scores = dot_t(query[span], key[upto])
                gap = lax.broadcasted_iota(jnp.int32, scores.shape, 0) - lax.broadcasted_iota(jnp.int32, scores.shape, 1) + i * part_rows
                decay = jnp.where(gap >= 0, jnp.exp(-rate * gap.astype(F32)), 0.0)
                o_buf[span, cols] = dot((scores * decay).astype(BF16), value[upto])
            to_end = (n_tok - 1 - lax.broadcasted_iota(jnp.int32, (n_tok, HEAD), 0)).astype(F32)
            faded = key.astype(F32) * jnp.exp(-rate * to_end)
            state[h] = dot(faded.T.astype(BF16), value)

        one_head(2 * pair)
        one_head(2 * pair + 1)

    def add_incoming():
        def head(h, carry):
            state[h] = state_in[h] * jnp.exp(jnp.zeros((HEAD, HEAD), F32) - slopes[h] * n_tok) + state[h]
            return carry

        lax.fori_loop(0, n_heads, head, 0)

    def send_state(batch):
        @pl.when(batch > 0)
        def _():
            pl.semaphore_wait(credit, 1)

        state_copy().start()

    def sq_copy(batch, k):
        peer = lax.rem(z + k, n_tp)
        return pltpu.make_async_remote_copy(
            src_ref=sq_send,
            dst_ref=sq_recv.at[batch, z],
            send_sem=sq_send_sem.at[k],
            recv_sem=sq_recv_sem.at[batch, z],
            device_id={"tp": peer},
            device_id_type=MESH,
        )

    def sq_arrival(batch, k):
        source = lax.rem(z + n_tp - k, n_tp)
        return pltpu.make_async_remote_copy(
            src_ref=sq_send,
            dst_ref=sq_recv.at[batch, source],
            send_sem=sq_send_sem.at[k],
            recv_sem=sq_recv_sem.at[batch, source],
            device_id={"tp": source},
            device_id_type=MESH,
        )

    def add_earlier(batch):
        @pl.when(c == n_cp - 1)
        def _():
            state_copy().wait_recv()

        @pl.when(c < n_cp - 1)
        def _():
            state_copy().wait_send()

        sq_acc[...] = jnp.zeros_like(sq_acc)

        def cols_of(h):
            return pl.ds(pl.multiple_of(h * HEAD, HEAD), HEAD)

        def head_pair(i, carry):
            for h in (2 * i, 2 * i + 1):
                steps = (lax.broadcasted_iota(jnp.int32, (n_tok, HEAD), 0) + 1).astype(F32)
                prior = dot(kvq[2, :, cols_of(h)], state_in[h].astype(BF16))
                vals = o_buf[:, cols_of(h)] + prior * jnp.exp(-slopes[h] * steps)
                o_buf[:, cols_of(h)] = vals
                sq_acc[...] += vals * vals
            return carry

        def head(h, carry):
            vals = o_buf[:, cols_of(h)]
            sq_acc[...] += vals * vals
            return carry

        @pl.when(c > 0)
        def _():
            lax.fori_loop(0, n_heads // 2, head_pair, 0)

        @pl.when(c == 0)
        def _():
            lax.fori_loop(0, n_heads, head, 0)

        @pl.when((c > 0) & (batch < n_batch - 1))
        def _():
            pl.semaphore_signal(credit, inc=1, device_id={"cp": c - 1}, device_id_type=MESH)

        row_sq = jnp.broadcast_to(jnp.sum(sq_acc[...], axis=-1, keepdims=True), (n_tok, HEAD))
        sq_send[...] = row_sq.T[0:8, :]
        sq_recv[batch, z] = sq_send[...]
        for k in range(1, n_tp):
            sq_copy(batch, k).start()

    def finish_lightning(batch):
        for k in range(1, n_tp):
            sq_arrival(batch, k).wait_recv()
        for k in range(1, n_tp):
            sq_copy(batch, k).wait_send()
        total = sq_recv[batch, 0]
        for k in range(1, n_tp):
            total = total + sq_recv[batch, k]
        tall = jnp.broadcast_to(total[0:1, :], (HEAD, n_tok)).T
        row_inv[...] = lax.rsqrt(tall / (width * n_tp) + NORM_EPS)

        def head(h, carry):
            cols = pl.ds(pl.multiple_of(h * HEAD, HEAD), HEAD)
            y_buf[:, cols] = (o_buf[:, cols] * row_inv[...] * ginner[h] * gate[:, cols]).astype(BF16)
            return carry

        lax.fori_loop(0, n_heads, head, 0)

    def unit_body(unit, carry):
        phase = lax.div(unit, UNITS) - 1
        r = lax.rem(unit, UNITS)
        which = lax.div(r, 8)
        tile = lax.rem(r, 8)
        first_layer = phase < n_batch - 1
        second_layer = (phase >= 3) & (phase < 3 + n_batch)
        projects = has_projection(phase)

        @pl.when(unit == 1)
        def _():
            pl.semaphore_wait(barrier, n_tp + n_cp - 2)

        @pl.when(lax.rem(tile, 3) == 0)
        def _():
            part_of = lax.div(tile, 3)

            def one(i, inner):
                service(phase * per_batch + which * per_group + part_of * (per_group // 3) + i)
                return inner

            if per_group == 3:
                one(0, 0)
            else:
                lax.fori_loop(0, per_group // 3, one, 0)

        @pl.when(lax.rem(r, 4) == 0)
        def _():
            @pl.when(phase <= 2)
            def _():
                for at_phase, at_r, batch in ((0, 0, 1), (1, 0, 2), (1, 20, 3)):

                    @pl.when((phase == at_phase) & (r == at_r))
                    def _():
                        hidden_copy(batch).wait()

                for at_phase, at_r, batch in ((-1, 4, 1), (0, 12, 2), (1, 12, 3)):

                    @pl.when((phase == at_phase) & (r == at_r))
                    def _():
                        hidden_copy(batch).start()

                @pl.when(r == 8)
                def _():
                    for i in range(2):
                        wo_copy(wo_a, i).start()

            @pl.when(second_layer)
            def _():
                @pl.when((r == 4) & (c == 1) | (r == 8) & (c == 2))
                def _():
                    state_copy().wait_recv()
                    add_incoming()
                    send_state(phase - 3)

                @pl.when(r == 8)
                def _():
                    for i in range(2):
                        wo_copy(wo_l, i).start()

                @pl.when(r == 12)
                def _():
                    add_earlier(phase - 3)

                @pl.when(r == 16)
                def _():
                    finish_lightning(phase - 3)

        @pl.when(first_layer & (r < 20))
        def _():
            later_start = jnp.where(phase <= 1, 10, 0)

            @pl.when(r == jnp.where(phase < 0, 9, later_start))
            def _():
                relay_kv(phase + 1)

            @pl.when(r == jnp.where(phase < 0, 12, later_start))
            def _():
                load_kv(phase + 1)

            k = r - 10
            by_five = lax.rem(r, 5)
            pair = jnp.where(phase < 0, 2 * (r - 12), jnp.where(phase <= 1, k - lax.div(k, 5), 2 * lax.div(r, 5) + (by_five == 2)))
            single = (phase >= 0) & (phase <= 1) & (r >= 10) & (by_five != 4) | (phase == 2) & ((by_five == 0) | (by_five == 2))
            n_here = jnp.where((phase < 0) & (r >= 12) & (r < 16), 2, jnp.where(single, 1, 0))

            def one_pair(i, inner):
                attend(phase + 1, pair + i)
                return inner

            lax.fori_loop(0, n_here, one_pair, 0)

        wo_tile = r - jnp.where(first_layer, 20, 16)

        @pl.when((wo_tile >= 0) & (wo_tile < n_wo) & (phase < 3 + n_batch))
        def _():
            out_project(phase, wo_tile)

            @pl.when((wo_tile < n_wo - 2) & first_layer)
            def _():
                wo_copy(wo_a, wo_tile + 2).start()

            @pl.when((wo_tile < n_wo - 2) & second_layer)
            def _():
                wo_copy(wo_l, wo_tile + 2).start()

        @pl.when(phase <= 1)
        def _():
            is_a, a_batch, a_j = a_tile(unit)

            @pl.when(is_a)
            def _():
                project_a(unit, a_batch, a_j)

        @pl.when(projects)
        def _():
            project_b(unit, lax.rem(phase, 2), which, tile)

            @pl.when(which == 3)
            def _():
                local_lightning(tile)

                @pl.when((tile == 7) & (c == 0))
                def _():
                    send_state(phase - 2)

        fetch(unit + W_SLOTS)
        return carry

    hidden_copy(0).wait()
    n_phases = 2 * n_batch + 2
    lax.fori_loop(0, n_phases * UNITS, unit_body, 0)
    for f in range(2):
        for k in range(4):
            out_copy(pieces - 4 + k, f, out).wait()


def copy_kernel(blocks, src, dst, buf, read_sem, write_sem):
    rows = src.shape[0] // blocks

    def read(i):
        span = pl.ds(i * rows, rows)
        return pltpu.make_async_copy(src.at[span, :], buf.at[span, :], read_sem.at[i])

    def write(i):
        span = pl.ds(i * rows, rows)
        return pltpu.make_async_copy(buf.at[span, :], dst.at[span, :], write_sem.at[i])

    for i in range(blocks):
        read(i).start()
    for i in range(blocks):
        read(i).wait()
        write(i).start()
    for i in range(blocks):
        write(i).wait()


def plain_copy(array, blocks):
    shape = jax.ShapeDtypeStruct(array.shape, array.dtype)
    return pl.pallas_call(
        functools.partial(copy_kernel, blocks),
        out_shape=shape,
        in_specs=[ANY],
        out_specs=ANY,
        scratch_shapes=[pltpu.VMEM(array.shape, array.dtype), pltpu.SemaphoreType.DMA((blocks,)), pltpu.SemaphoreType.DMA((blocks,))],
        compiler_params=pltpu.CompilerParams(vmem_limit_bytes=48 * 1024 * 1024),
    )(array)


def fused_layers(hid, weights, gains, ginner, alphas, slopes, n_tok, n_tp, n_cp):
    n_rows, model = hid.shape
    width = weights[2].shape[1]
    kv_width = weights[0].shape[1]
    n_batch = n_rows // n_tok
    n_heads = width // HEAD
    rows = n_tok // 24
    w_cols = width // 8
    wo_cols = model // 12
    vmem, dma = pltpu.VMEM, pltpu.SemaphoreType.DMA
    scratch = [
        vmem((2, n_tok, model), BF16),
        vmem((2, n_tok, model), BF16),
        vmem((2, n_tok, model), BF16),
        vmem((W_SLOTS, model, w_cols), BF16),
        vmem((2, width, wo_cols), BF16),
        vmem((n_tok, width), BF16),
        vmem((3, n_tok, width), BF16),
        vmem((n_tok, width), F32),
        vmem((n_tok, width), F32),
        vmem((n_heads, HEAD, HEAD), F32),
        vmem((n_heads, HEAD, HEAD), F32),
        vmem((2, 4, rows, model), BF16),
        vmem((2, rows, model), F32),
        vmem((2, 1, model), F32),
        vmem((n_tok, w_cols), F32),
        vmem((n_tok, HEAD), F32),
        vmem((n_tok, HEAD), F32),
        vmem((8, n_tok), F32),
        vmem((n_batch, n_tp, 8, n_tok), F32),
        vmem((n_tok, 2 * kv_width), BF16),
        vmem((n_cp, n_tok, 2 * kv_width), BF16),
        vmem((3, n_tok, HEAD), F32),
        vmem((2, n_tok, HEAD), F32),
        dma((2, RING)),
        dma((2, RING)),
        dma((2, RING)),
        dma((2, RING)),
        dma((2, 4)),
        dma((2, 4)),
        dma((W_SLOTS,)),
        dma((2,)),
        dma((2,)),
        dma,
        dma((n_cp,)),
        dma((n_batch, n_cp)),
        dma((n_cp + 1,)),
        dma,
        dma,
        dma((n_tp,)),
        dma((n_batch, n_tp)),
        pltpu.SemaphoreType.REGULAR,
    ]
    flops = 2 * n_rows * model * width * 8
    return pl.pallas_call(
        functools.partial(fused_kernel, n_tp, n_cp),
        out_shape=[
            jax.ShapeDtypeStruct((n_rows, model), BF16),
            jax.ShapeDtypeStruct((n_rows, model), BF16),
            jax.ShapeDtypeStruct((n_batch, n_cp, n_tok, 2 * kv_width), BF16),
        ],
        in_specs=[ANY] * 11 + [VMEM] * 3 + [SMEM] * 2,
        out_specs=[ANY] * 3,
        scratch_shapes=scratch,
        compiler_params=pltpu.CompilerParams(collective_id=0, has_side_effects=True, vmem_limit_bytes=67043328),
        cost_estimate=pl.CostEstimate(flops=flops, bytes_accessed=12 * n_rows * model, transcendentals=0),
    )(hid, *weights, rotary_table(n_tok * n_cp), *gains, ginner, alphas, slopes)


def solution(mesh):
    n_tp, n_cp = mesh.shape["tp"], mesh.shape["cp"]

    def body(hidden, alphas, wq_attn, wk_attn, wv_attn, wo_attn, gain_attn, wq_lin, wk_lin, wv_lin, wg_lin, slopes, gain_inner, wo_lin, gain_lin):
        n_batch, n_tok, model = hidden.shape
        flat = hidden.reshape(n_batch * n_tok, model)
        gains = (gain_attn[None, :], gain_lin[None, :])
        weights = (wk_attn, wv_attn, wq_attn, wo_attn, wk_lin, wv_lin, wq_lin, wg_lin, wo_lin)
        outs = fused_layers(flat, weights, gains, gain_inner.reshape(-1, 1, HEAD), alphas, slopes, n_tok, n_tp, n_cp)
        return plain_copy(outs[0], 16).reshape(hidden.shape)

    act_spec = P("dp", "cp", None)
    rep_spec = P()
    col_spec = P(None, "tp")
    row_spec = P("tp", None)
    vec_spec = P("tp")
    in_specs = (act_spec, rep_spec, col_spec, col_spec, col_spec, row_spec, rep_spec, col_spec, col_spec, col_spec, col_spec, vec_spec, vec_spec, row_spec, rep_spec)
    return jax.shard_map(body, mesh=mesh, in_specs=in_specs, out_specs=act_spec, check_vma=False)
```
